32 devices in a mesh: gz: 2 (over y), row: 4 (over z), col: 4 (over x, core).
Axes of the slice: x: 2, y: 2, z: 4, core: 2. Of those that a mesh axis runs over, the one named last changes fastest.
Arguments:
- lpanel: bfloat16 [2, 2, 1024, 2048], P(None, 'gz', 'row', 'col'), may hold values from -6 to 6
- upanel: bfloat16 [2, 2, 2048, 4096], P(None, 'gz', 'row', 'col'), may hold values from -0.125 to 0.125
- rowmap: int32 [2, 2, 4], P(None, 'gz', 'row'), may hold values from 0 to 1
- colmap: int32 [2, 2, 16], P(None, 'gz', 'col'), may hold values from 0 to 1
- blockmask: int32 [2, 2, 4, 16], P(None, 'gz', 'row', 'col'), may hold values 0 or 1
- front_blocks: bfloat16 [2, 2048, 2048], P(None, 'row', ('gz', 'col')), may hold values from -6 to 6
Outputs:
- front_update: bfloat16 [2, 2048, 2048], P(None, 'row', ('gz', 'col'))
The draws below stay inside these ranges and needn't reach their ends.
All inputs are finite; a program needn't handle non-finite values. No bound on the sum of `blockmask` on one device may be relied on, other than what follows from the above.
Results may differ from the reference program's by a relative error of at most 0.008.
Values may be sent and summed in bfloat16 or wider, within the bound.
A program may use at most 64 MiB of HBM per device.

```python
import math
import jax
import jax.numpy as jnp
import numpy as np
from jax import lax

B = 256
W = 2048
CB = 4
FRB = 2
LEVELS = 2
UR = 1024
UC = 4096
FR = 2048
FC = 2048
N_GZ = 2
N_ROW = 4
N_COL = 4


def set_ends(values, rng, low, top_value):
    extent = values.shape
    place = [jax.random.randint(jax.random.fold_in(rng, axis), (), 0, extent[axis]) for axis in range(len(extent))]
    values = values.at[tuple(place)].set(low)
    longest = extent.index(max(extent))
    place[longest] = (place[longest] + 1) % extent[longest]
    return values.at[tuple(place)].set(top_value)


def level_of(rng, extent, cuts, least, top_value):
    gain = 1.0
    for position, blocks in cuts:
        draws = jax.random.uniform(jax.random.fold_in(jax.random.fold_in(rng, 6), position), (blocks,), jnp.float32, least / len(cuts), top_value / len(cuts))
        gain = gain * jnp.repeat(jnp.exp(draws), extent[position] // blocks).reshape((-1,) + (1,) * (len(extent) - 1 - position))
    return gain


def rank_bounds(amount, slope):
    portions = [(1 << 20) // math.isqrt(standing ** slope) + 1 for standing in range(1, amount + 1)]
    spread = 1 + sum(portions) // (1 << 30)
    return np.cumsum(np.array([max(1, weight // spread) for weight in portions]))


def ranked(own_key, extent, amount, slope):
    table = rank_bounds(amount, slope)
    pick = jax.random.randint(jax.random.fold_in(own_key, 1), extent, 0, int(table[amount - 1]))
    rank = jnp.searchsorted(jnp.asarray(table, jnp.int32), pick, side="right")
    return jax.random.permutation(jax.random.fold_in(own_key, 2), amount)[rank].astype(jnp.int32)


def gaussian(rng, shape, width, limit, pieces=(), kind=jnp.bfloat16):
    values = jax.random.normal(rng, shape, jnp.float32) * width
    if len(pieces) > 0:
        values = level_of(rng, shape, pieces, -0.22, 0.18) * values
    return jnp.clip(values, min=-limit, max=limit).astype(kind)


def setup_inputs(seed: int = 0) -> dict:
    key_list = jax.random.split(jax.random.key(seed), 7)
    lpanel = gaussian(key_list[0], (LEVELS, N_GZ, UR, W), 1.0, 6.0, ((1, 2), (2, 4), (3, 4)))
    upanel = gaussian(key_list[1], (LEVELS, N_GZ, W, UC), W ** -0.5, 0.125, ((1, 2), (2, 4), (3, 4)))
    rowmap = set_ends(jax.random.randint(key_list[2], (LEVELS, N_GZ, N_ROW), 0, FRB), jax.random.fold_in(key_list[2], 1), 0, FRB - 1).astype(jnp.int32)
    colmap = set_ends(ranked(key_list[3], (LEVELS, N_GZ, N_COL * CB), N_GZ, 2), jax.random.fold_in(key_list[3], 3), 0, N_GZ - 1).astype(jnp.int32)
    blockmask = set_ends((jax.random.randint(key_list[4], (LEVELS, N_GZ, N_ROW, N_COL * CB), 0, 4) < 3).astype(jnp.int32), jax.random.fold_in(key_list[4], 1), 0, 1)
    front_blocks = gaussian(key_list[5], (LEVELS, FR, FC), 1.0, 6.0, ((1, 4), (2, 8)))
    return dict(lpanel=lpanel, upanel=upanel, rowmap=rowmap, colmap=colmap, blockmask=blockmask, front_blocks=front_blocks)


def layer_partial(schur, rows_of, cols_of, live):
    blocks = schur.reshape(N_ROW, B, N_COL, CB, B)
    targets = cols_of.reshape(N_COL, CB)[:, :, None] == jnp.arange(N_GZ, dtype=jnp.int32)[None, None, :]
    col_select = targets.astype(jnp.float32)[None] * live.reshape(N_ROW, N_COL, CB).astype(jnp.float32)[:, :, :, None]
    col_sums = jnp.einsum("rbcjk,rcjl->rblck", blocks, col_select, precision=lax.Precision.HIGHEST)
    row_select = (rows_of[:, None] == jnp.arange(FRB, dtype=jnp.int32)[None, :]).astype(jnp.float32)
    placed = row_select[:, :, None, None, None, None] * col_sums[:, None]
    return placed.reshape(FR, FC)


def reference(lpanel, upanel, rowmap, colmap, blockmask, front_blocks):
    results = []
    for depth in range(LEVELS):
        total = jnp.zeros((FR, FC), jnp.float32)
        for layer in range(N_GZ):
            schur = jnp.dot(lpanel[depth, layer], upanel[depth, layer], preferred_element_type=jnp.float32)
            partial_value = layer_partial(schur, rowmap[depth, layer], colmap[depth, layer], blockmask[depth, layer])
            total = total + partial_value.astype(jnp.bfloat16).astype(jnp.float32)
        results.append((front_blocks[depth].astype(jnp.float32) - total).astype(jnp.bfloat16))
    return jnp.stack(results)
```

```python
import functools

import jax
import jax.numpy as jnp
from jax import lax
from jax.experimental import pallas as pl
from jax.experimental.pallas import tpu as pltpu
from jax.sharding import PartitionSpec as P

CB = 4
FRB = 2
MESH = pl.DeviceIdType.MESH


def column_sums(schur, cols_of, live, layers):
    width = schur.shape[0]
    blocks = schur.reshape(width, CB, width)
    targets = cols_of[:, None] == jnp.arange(layers, dtype=jnp.int32)[None, :]
    col_select = targets.astype(jnp.float32) * live.astype(jnp.float32)[:, None]
    return jnp.einsum("bjk,jl->lbk", blocks, col_select, precision=lax.Precision.HIGHEST)


def general(lpanel, upanel, rowmap, colmap, blockmask, front_blocks):
    layers = lax.axis_size("gz")
    width = lpanel.shape[2]
    levels = lpanel.shape[0]
    tiles = []
    for depth in range(levels):
        left_rows = lax.all_gather(lpanel[depth, 0], "col", axis=1, tiled=True)
        tiles.append(
            jnp.dot(
                left_rows,
                lax.all_gather(upanel[depth, 0], "row", axis=0, tiled=True),
                preferred_element_type=jnp.float32,
            )
        )
    results = []
    every_row = lax.all_gather(rowmap[:, :, 0], "gz", axis=1, tiled=True)
    for depth in range(levels):
        sums = column_sums(tiles[depth], colmap[depth, 0], blockmask[depth, 0, 0], layers).astype(
            jnp.bfloat16
        )
        arrived = lax.all_to_all(sums, "gz", split_axis=0, concat_axis=0, tiled=True)
        row_select = (
            every_row[depth][:, None] == jnp.arange(FRB, dtype=jnp.int32)[None, :]
        ).astype(jnp.float32)
        placed = jnp.einsum(
            "sf,sbk->fbk", row_select, arrived.astype(jnp.float32), precision=lax.Precision.HIGHEST
        )
        placed = placed.reshape(FRB * width, width)
        results.append((front_blocks[depth].astype(jnp.float32) - placed).astype(jnp.bfloat16))
    return jnp.stack(results)


def kernel(
    rows, cols, layers, levels, width,
    l_hbm, u_hbm, cm_ref, live_ref, rm_ref, front_hbm, out_ref,
    l_ref, u_ref, front_ref, crossed, l_all, live_all, own, part, p_in, y_out, y_in, rm_in,
    in_sem, own_sem, x_send, x_recv, c_send, l_send, l_recv, post_send, relay_send,
    m_send, m_recv, m_loc, p_send, p_recv, y_send, y_recv, rm_send, rm_recv,
):
    z = lax.axis_index("row")
    c = lax.axis_index("col")
    g = lax.axis_index("gz")
    far = lax.rem(c + cols // 2, cols)
    mate = c + 1 - 2 * lax.rem(c, 2)
    other = 1 - g
    last = rows - 1
    entry, second = c == z, far == z
    gate = jnp.logical_or(entry, second)
    low = 1 - z // (rows // 2)
    depth = low * z + (1 - low) * (last - z)
    at_end = depth == 0
    inner = jnp.logical_not(at_end)

    def remote(src, dst, send, recv, where):
        return pltpu.make_async_remote_copy(
            src_ref=src, dst_ref=dst, send_sem=send, recv_sem=recv,
            device_id=where, device_id_type=MESH,
        )

    first = pltpu.make_async_copy(l_hbm, l_ref, in_sem.at[0])
    first.start()
    whole_u = pltpu.make_async_copy(u_hbm, u_ref, in_sem.at[1])
    whole_u.start()
    fronts = pltpu.make_async_copy(front_hbm, front_ref, in_sem.at[2])
    fronts.start()

    def own_load(v):
        return pltpu.make_async_copy(l_hbm.at[v], l_all.at[v, z], own_sem.at[v])

    @pl.when(entry)
    def _():
        for v in range(levels):
            own_load(v).start()

    barrier = pltpu.get_barrier_semaphore()
    for step in range(1, rows):
        pl.semaphore_signal(
            barrier, inc=1, device_id={"row": lax.rem(z + step, rows)}, device_id_type=MESH
        )
    pl.semaphore_signal(barrier, inc=1, device_id={"col": far}, device_id_type=MESH)
    pl.semaphore_signal(barrier, inc=1, device_id={"col": mate}, device_id_type=MESH)
    pl.semaphore_signal(barrier, inc=1, device_id={"gz": other}, device_id_type=MESH)
    first.wait()
    pl.semaphore_wait(barrier, rows + 2)

    half = width // 2
    pieces = [slice(h * half, (h + 1) * half) for h in range(2)]

    def via(r, q):
        lo = 1 - r // (rows // 2)
        rr = lo * r + (1 - lo) * (last - r)
        qq = lo * q + (1 - lo) * (last - q)
        return jnp.logical_and(qq >= 2, jnp.logical_or(rr == 1, qq == 2))

    def place(v, h):
        return remote(
            l_ref.at[v, pieces[h]], l_all.at[v, z, pieces[h]],
            l_send.at[v, h], l_recv.at[v, h, z], {"row": c},
        )

    def cross(v):
        return remote(
            l_ref.at[v, pieces[1]], crossed.at[v], x_send.at[v], x_recv.at[v], {"col": far}
        )

    def onward(v):
        return remote(
            crossed.at[v], l_all.at[v, z, pieces[1]], c_send.at[v], l_recv.at[v, 1, z], {"row": far}
        )

    via_here, via_far = via(z, c), via(z, far)
    away = jnp.logical_not(entry)
    straight = jnp.logical_and(away, jnp.logical_not(via_here))

    for v in range(levels):
        pl.when(via_here)(lambda v=v: cross(v).start())
        pl.when(away)(lambda v=v: place(v, 0).start())
        pl.when(straight)(lambda v=v: place(v, 1).start())

    own_live = pltpu.make_async_copy(live_ref, live_all.at[z], m_loc)
    own_live.start()
    live_out = []
    for step in range(1, rows):
        to = lax.rem(z + step, rows)
        live_out.append(
            remote(live_ref, live_all.at[z], m_send.at[step], m_recv.at[z], {"row": to})
        )
        live_out[-1].start()
    rm_copy = remote(rm_ref, rm_in, rm_send, rm_recv, {"gz": other})
    rm_copy.start()

    def carry_on(v):
        @pl.when(via_far)
        def _():
            cross(v).wait_recv()
            onward(v).start()

    def passes(v, a, h):
        spot = l_all.at[v, a, pieces[h]]
        post = remote(spot, spot, post_send.at[v, h, a], l_recv.at[v, h, a], {"col": far})
        relay = remote(spot, spot, relay_send.at[v, h, a], l_recv.at[v, h, a], {"col": mate})
        return post, relay

    count = rows - 1

    def place_of(k):
        mine = k // (levels * count)
        i = lax.rem(k, count)
        near = (1 - depth) * (i + 1) + depth * (i + (i + 1) // 2)
        near = low * near + (1 - low) * (last - near)
        v = mine * (k - levels * count) + (1 - mine) * (k // count)
        return v, mine * z + (1 - mine) * near

    def gather(k):
        v, a = place_of(k)
        turned = via(a, z)

        def spread(h):
            post, relay = passes(v, a, h)
            post.start()
            relay.start()

        @pl.when(entry)
        def _():
            pl.when(a == z)(lambda: own_load(v).wait())
            pl.when(a != z)(lambda: passes(v, a, 0)[1].wait_recv())
            spread(0)

            @pl.when(jnp.logical_not(turned))
            def _():
                pl.when(a != z)(lambda: passes(v, a, 1)[1].wait_recv())
                spread(1)

        @pl.when(jnp.logical_and(second, turned))
        def _():
            passes(v, a, 1)[1].wait_recv()
            spread(1)

    def take(k):
        v, a = place_of(k)
        turned = via(a, z)

        def hand(h):
            relay = passes(v, a, h)[1]
            relay.wait_recv()
            relay.start()

        pl.when(second)(lambda: hand(0))
        pl.when(jnp.logical_and(second, jnp.logical_not(turned)))(lambda: hand(1))
        pl.when(jnp.logical_and(entry, turned))(lambda: hand(1))

        @pl.when(jnp.logical_not(gate))
        def _():
            for h in range(2):
                passes(v, a, h)[1].wait_recv()

    def hop(v, a, l, side, to):
        return remote(
            part.at[v, a, l], p_in.at[v, side, a, l],
            p_send.at[v, a, l], p_recv.at[v, side, a, l], {"row": to},
        )

    inward, outward = 1 - low, low
    near_end, far_end = last * inward, last * low
    across_mid = last - z
    next_in = low + (1 - low) * (last - 1)

    def send(v, a, l):
        part[v, a, l] = own[v, a, l].astype(jnp.bfloat16)
        hop(v, a, l, inward, next_in).start()

    def item(k):
        v, a = place_of(k)
        block = l_all[v, a]
        to_layer = cm_ref[v]
        live = live_all[a, v]
        for j in range(CB):
            t = jnp.dot(
                block, u_ref[v, :, j * width : (j + 1) * width], preferred_element_type=jnp.float32
            )
            for l in range(layers):
                m = jnp.where(to_layer[:, j : j + 1] == l, live[:, j : j + 1], 0).astype(jnp.float32)
                if j == 0:
                    own[v, a, l] = t * m
                else:
                    own[v, a, l] += t * m

        @pl.when(jnp.logical_and(at_end, k < count))
        def _():
            send(v, a, other)
            pl.when(k > 0)(lambda: send(v, a, g))

        @pl.when(jnp.logical_and(at_end, k == levels * count - 1))
        def _():
            late = levels - 1
            near, mid, end = next_in, last - next_in, last - z
            for a_, l_ in ((end, other), (mid, other), (end, g), (near, other), (mid, g)):
                send(late, a_, l_)
            send(0, near, g)
            send(late, near, g)

    carry_on(0)
    gather(0)
    own_live.wait()
    for step in range(1, rows):
        src = lax.rem(z + step, rows)
        remote(live_ref, live_all.at[src], m_send.at[step], m_recv.at[src], {"row": src}).wait_recv()
    whole_u.wait()
    total = levels * rows

    def body(k, carry):
        pl.when(k == 0)(lambda: [carry_on(v) for v in range(1, levels)] and None)
        pl.when(k < total - 1)(lambda: gather(k + 1))
        take(k)
        item(k)
        return carry

    lax.fori_loop(0, total, body, 0)

    def collect(v, l, side):
        hop(v, z, l, side, z).wait_recv()
        own[v, z, l] += p_in[v, side, z, l].astype(jnp.float32)

    def forward(v, a, l, side, to):
        hop(v, a, l, side, to).wait_recv()
        part[v, a, l] = (own[v, a, l] + p_in[v, side, a, l].astype(jnp.float32)).astype(jnp.bfloat16)
        hop(v, a, l, side, to).start()

    def way(v):
        return remote(y_out.at[v], y_in.at[v], y_send.at[v], y_recv.at[v], {"gz": other})

    def trade(v):
        y_out[v] = own[v, z, other].astype(jnp.bfloat16)
        way(v).start()

    def finish(v):
        mine = own[v, z, g].astype(jnp.bfloat16).astype(jnp.float32)
        way(v).wait_recv()
        theirs = y_in[v].astype(jnp.float32)
        for f in range(FRB):
            lines = slice(f * width, (f + 1) * width)
            here = (rm_ref[v] == f).astype(jnp.float32)
            there = (rm_in[v] == f).astype(jnp.float32)
            total = here * mine + there * theirs
            out_ref[v, lines, :] = (front_ref[v, lines, :].astype(jnp.float32) - total).astype(
                out_ref.dtype
            )

    fronts.wait()
    rm_copy.wait()

    @pl.when(at_end)
    def _():
        collect(0, other, outward)
        trade(0)
        collect(0, g, outward)
        collect(1, other, outward)
        trade(1)
        finish(0)
        collect(1, g, outward)

    @pl.when(inner)
    def _():
        def ahead(v, a, l):
            forward(v, a, l, inward, across_mid)

        def back(v, l):
            forward(v, near_end, l, outward, near_end)

        collect(0, other, inward)
        ahead(0, across_mid, other)
        ahead(0, across_mid, g)
        collect(0, other, outward)
        trade(0)
        ahead(0, far_end, other)
        collect(0, g, outward)
        ahead(0, far_end, g)
        back(0, other)
        ahead(1, far_end, other)
        back(0, g)
        ahead(1, across_mid, other)
        back(1, other)
        ahead(1, far_end, g)
        collect(1, other, outward)
        collect(1, other, inward)
        trade(1)
        back(1, g)
        ahead(1, across_mid, g)
        collect(0, g, inward)
        finish(0)
        collect(1, g, outward)
        collect(1, g, inward)

    finish(1)

    for copy in live_out:
        copy.wait_send()
    for v in range(levels):
        way(v).wait_send()
        pl.when(via_here)(cross(v).wait_send)
        pl.when(via_far)(onward(v).wait_send)
        pl.when(away)(place(v, 0).wait_send)
        pl.when(straight)(place(v, 1).wait_send)

        def drain(a, carry, v=v):
            turned = via(a, z)

            @pl.when(gate)
            def _():
                for h in range(2):
                    passes(v, a, h)[1].wait_send()

            pl.when(entry)(lambda: passes(v, a, 0)[0].wait_send())
            posted = jnp.logical_or(
                jnp.logical_and(entry, jnp.logical_not(turned)), jnp.logical_and(second, turned)
            )
            pl.when(posted)(lambda: passes(v, a, 1)[0].wait_send())

            @pl.when(a != z)
            def _():
                for l in range(layers):
                    hop(v, a, l, 0, z).wait_send()

            return carry

        lax.fori_loop(0, rows, drain, 0)


def stationary(rows, cols, layers, lpanel, upanel, rowmap, colmap, blockmask, front_blocks):
    levels, _, width, depth = lpanel.shape
    bf16 = jnp.bfloat16
    vmem = pl.BlockSpec(memory_space=pltpu.VMEM)
    hbm = pl.BlockSpec(memory_space=pl.ANY)
    dma = pltpu.SemaphoreType.DMA
    return pl.pallas_call(
        functools.partial(kernel, rows, cols, layers, levels, width),
        out_shape=jax.ShapeDtypeStruct(front_blocks.shape, front_blocks.dtype),
        in_specs=[hbm, hbm, vmem, vmem, vmem, hbm],
        out_specs=vmem,
        scratch_shapes=[
            pltpu.VMEM((levels, width, depth), bf16),
            pltpu.VMEM(upanel[:, 0].shape, bf16),
            pltpu.VMEM(front_blocks.shape, bf16),
            pltpu.VMEM((levels, width // 2, depth), bf16),
            pltpu.VMEM((levels, rows, width, depth), bf16),
            pltpu.VMEM((rows,) + blockmask.shape[:1] + blockmask.shape[2:], jnp.int32),
            pltpu.VMEM((levels, rows, layers, width, width), jnp.float32),
            pltpu.VMEM((levels, rows, layers, width, width), bf16),
            pltpu.VMEM((levels, 2, rows, layers, width, width), bf16),
            pltpu.VMEM((levels, width, width), bf16),
            pltpu.VMEM((levels, width, width), bf16),
            pltpu.VMEM(rowmap.shape, jnp.int32),
            dma((3,)),
            dma((levels,)),
            dma((levels,)),
            dma((levels,)),
            dma((levels,)),
            dma((levels, 2)),
            dma((levels, 2, rows)),
            dma((levels, 2, rows)),
            dma((levels, 2, rows)),
            dma((rows,)),
            dma((rows,)),
            dma,
            dma((levels, rows, layers)),
            dma((levels, 2, rows, layers)),
            dma((levels,)),
            dma((levels,)),
            dma,
            dma,
        ],
        compiler_params=pltpu.CompilerParams(collective_id=0, has_side_effects=True),
    )(lpanel[:, 0], upanel[:, 0], colmap, blockmask[:, 0], rowmap, front_blocks)


def solution(mesh):
    rows, cols, layers = mesh.shape["row"], mesh.shape["col"], mesh.shape["gz"]
    body = general
    if rows == cols == 2 * layers and layers == 2:
        body = functools.partial(stationary, rows, cols, layers)
    return jax.shard_map(
        body,
        mesh=mesh,
        in_specs=(
            P(None, "gz", "row", "col"),
            P(None, "gz", "row", "col"),
            P(None, "gz", "row"),
            P(None, "gz", "col"),
            P(None, "gz", "row", "col"),
            P(None, "row", ("gz", "col")),
        ),
        out_specs=P(None, "row", ("gz", "col")),
        check_vma=False,
    )
```

```python
import functools

import jax
import jax.numpy as jnp
from jax import lax
from jax.experimental import pallas as pl
from jax.experimental.pallas import tpu as pltpu
from jax.sharding import PartitionSpec as P

CB = 4
FRB = 2
MESH = pl.DeviceIdType.MESH


def column_sums(schur, cols_of, live, layers):
    width = schur.shape[0]
    blocks = schur.reshape(width, CB, width)
    targets = cols_of[:, None] == jnp.arange(layers, dtype=jnp.int32)[None, :]
    col_select = targets.astype(jnp.float32) * live.astype(jnp.float32)[:, None]
    return jnp.einsum("bjk,jl->lbk", blocks, col_select, precision=lax.Precision.HIGHEST)


def general(lpanel, upanel, rowmap, colmap, blockmask, front_blocks):
    layers = lax.axis_size("gz")
    width = lpanel.shape[2]
    levels = lpanel.shape[0]
    tiles = []
    for depth in range(levels):
        left_rows = lax.all_gather(lpanel[depth, 0], "col", axis=1, tiled=True)
        tiles.append(
            jnp.dot(
                left_rows,
                lax.all_gather(upanel[depth, 0], "row", axis=0, tiled=True),
                preferred_element_type=jnp.float32,
            )
        )
    results = []
    every_row = lax.all_gather(rowmap[:, :, 0], "gz", axis=1, tiled=True)
    for depth in range(levels):
        sums = column_sums(tiles[depth], colmap[depth, 0], blockmask[depth, 0, 0], layers).astype(
            jnp.bfloat16
        )
        arrived = lax.all_to_all(sums, "gz", split_axis=0, concat_axis=0, tiled=True)
        row_select = (
            every_row[depth][:, None] == jnp.arange(FRB, dtype=jnp.int32)[None, :]
        ).astype(jnp.float32)
        placed = jnp.einsum(
            "sf,sbk->fbk", row_select, arrived.astype(jnp.float32), precision=lax.Precision.HIGHEST
        )
        placed = placed.reshape(FRB * width, width)
        results.append((front_blocks[depth].astype(jnp.float32) - placed).astype(jnp.bfloat16))
    return jnp.stack(results)


def kernel(
    rows, cols, layers, levels, width,
    l_hbm, u_hbm, cm_ref, live_ref, rm_ref, front_hbm, out_ref,
    l_ref, u_ref, front_ref, crossed, l_all, live_all, own, part, p_in, y_out, y_in, rm_in,
    in_sem, own_sem, x_send, x_recv, c_send, l_send, l_recv, post_send, relay_send,
    m_send, m_recv, m_loc, p_send, p_recv, y_send, y_recv, rm_send, rm_recv,
):
    z = lax.axis_index("row")
    c = lax.axis_index("col")
    g = lax.axis_index("gz")
    far = lax.rem(c + cols // 2, cols)
    mate = c + 1 - 2 * lax.rem(c, 2)
    other = 1 - g
    last = rows - 1
    entry, second = c == z, far == z
    gate = jnp.logical_or(entry, second)
    low = 1 - z // (rows // 2)
    depth = low * z + (1 - low) * (last - z)
    at_end = depth == 0
    inner = jnp.logical_not(at_end)

    def remote(src, dst, send, recv, where):
        return pltpu.make_async_remote_copy(
            src_ref=src, dst_ref=dst, send_sem=send, recv_sem=recv,
            device_id=where, device_id_type=MESH,
        )

    first = pltpu.make_async_copy(l_hbm, l_ref, in_sem.at[0])
    first.start()
    whole_u = pltpu.make_async_copy(u_hbm, u_ref, in_sem.at[1])
    whole_u.start()
    fronts = pltpu.make_async_copy(front_hbm, front_ref, in_sem.at[2])
    fronts.start()

    def own_load(v):
        return pltpu.make_async_copy(l_hbm.at[v], l_all.at[v, z], own_sem.at[v])

    @pl.when(entry)
    def _():
        for v in range(levels):
            own_load(v).start()

    barrier = pltpu.get_barrier_semaphore()
    for step in range(1, rows):
        pl.semaphore_signal(
            barrier, inc=1, device_id={"row": lax.rem(z + step, rows)}, device_id_type=MESH
        )
    pl.semaphore_signal(barrier, inc=1, device_id={"col": far}, device_id_type=MESH)
    pl.semaphore_signal(barrier, inc=1, device_id={"col": mate}, device_id_type=MESH)
    pl.semaphore_signal(barrier, inc=1, device_id={"gz": other}, device_id_type=MESH)
    first.wait()
    pl.semaphore_wait(barrier, rows + 2)

    half = width // 2
    pieces = [slice(h * half, (h + 1) * half) for h in range(2)]

    def via(r, q):
        lo = 1 - r // (rows // 2)
        rr = lo * r + (1 - lo) * (last - r)
        qq = lo * q + (1 - lo) * (last - q)
        return jnp.logical_and(qq >= 2, jnp.logical_or(rr == 1, qq == 2))

    def place(v, h):
        return remote(
            l_ref.at[v, pieces[h]], l_all.at[v, z, pieces[h]],
            l_send.at[v, h], l_recv.at[v, h, z], {"row": c},
        )

    def cross(v):
        return remote(
            l_ref.at[v, pieces[1]], crossed.at[v], x_send.at[v], x_recv.at[v], {"col": far}
        )

    def onward(v):
        return remote(
            crossed.at[v], l_all.at[v, z, pieces[1]], c_send.at[v], l_recv.at[v, 1, z], {"row": far}
        )

    via_here, via_far = via(z, c), via(z, far)
    away = jnp.logical_not(entry)
    straight = jnp.logical_and(away, jnp.logical_not(via_here))

    def launch(v):
        pl.when(via_here)(lambda: cross(v).start())
        pl.when(away)(lambda: place(v, 0).start())
        pl.when(straight)(lambda: place(v, 1).start())

    launch(0)
    pl.when(at_end)(lambda: launch(1))

    own_live = pltpu.make_async_copy(live_ref, live_all.at[z], m_loc)
    own_live.start()
    live_out = []
    for step in range(1, rows):
        to = lax.rem(z + step, rows)
        live_out.append(
            remote(live_ref, live_all.at[z], m_send.at[step], m_recv.at[z], {"row": to})
        )
        live_out[-1].start()
    rm_copy = remote(rm_ref, rm_in, rm_send, rm_recv, {"gz": other})
    rm_copy.start()

    def carry_on(v):
        @pl.when(via_far)
        def _():
            cross(v).wait_recv()
            onward(v).start()

    def passes(v, a, h):
        spot = l_all.at[v, a, pieces[h]]
        post = remote(spot, spot, post_send.at[v, h, a], l_recv.at[v, h, a], {"col": far})
        relay = remote(spot, spot, relay_send.at[v, h, a], l_recv.at[v, h, a], {"col": mate})
        return post, relay

    count = rows - 1

    def place_of(k):
        mine = k // (levels * count)
        i = lax.rem(k, count)
        near = (1 - depth) * (i + 1) + depth * (i + (i + 1) // 2)
        near = low * near + (1 - low) * (last - near)
        v = mine * (k - levels * count) + (1 - mine) * (k // count)
        return v, mine * z + (1 - mine) * near

    def gather(k):
        v, a = place_of(k)
        turned = via(a, z)

        def spread(h):
            post, relay = passes(v, a, h)
            post.start()
            relay.start()

        @pl.when(entry)
        def _():
            pl.when(a == z)(lambda: own_load(v).wait())
            pl.when(a != z)(lambda: passes(v, a, 0)[1].wait_recv())
            spread(0)

            @pl.when(jnp.logical_not(turned))
            def _():
                pl.when(a != z)(lambda: passes(v, a, 1)[1].wait_recv())
                spread(1)

        @pl.when(jnp.logical_and(second, turned))
        def _():
            passes(v, a, 1)[1].wait_recv()
            spread(1)

    def take(k):
        v, a = place_of(k)
        turned = via(a, z)

        def hand(h):
            relay = passes(v, a, h)[1]
            relay.wait_recv()
            relay.start()

        pl.when(second)(lambda: hand(0))
        pl.when(jnp.logical_and(second, jnp.logical_not(turned)))(lambda: hand(1))
        pl.when(jnp.logical_and(entry, turned))(lambda: hand(1))

        @pl.when(jnp.logical_not(gate))
        def _():
            for h in range(2):
                passes(v, a, h)[1].wait_recv()

    def hop(v, a, l, side, to):
        return remote(
            part.at[v, a, l], p_in.at[v, side, a, l],
            p_send.at[v, a, l], p_recv.at[v, side, a, l], {"row": to},
        )

    inward, outward = 1 - low, low
    near_end, far_end = last * inward, last * low
    across_mid = last - z
    next_in = low + (1 - low) * (last - 1)

    def send(v, a, l):
        part[v, a, l] = own[v, a, l].astype(jnp.bfloat16)
        hop(v, a, l, inward, next_in).start()

    def item(k):
        v, a = place_of(k)
        block = l_all[v, a]
        to_layer = cm_ref[v]
        live = live_all[a, v]
        for j in range(CB):
            t = jnp.dot(
                block, u_ref[v, :, j * width : (j + 1) * width], preferred_element_type=jnp.float32
            )
            for l in range(layers):
                m = jnp.where(to_layer[:, j : j + 1] == l, live[:, j : j + 1], 0).astype(jnp.float32)
                if j == 0:
                    own[v, a, l] = t * m
                else:
                    own[v, a, l] += t * m


    carry_on(0)
    pl.when(at_end)(lambda: carry_on(1))
    gather(0)
    own_live.wait()
    for step in range(1, rows):
        src = lax.rem(z + step, rows)
        remote(live_ref, live_all.at[src], m_send.at[step], m_recv.at[src], {"row": src}).wait_recv()
    whole_u.wait()
    rm_copy.wait()
    fronts.wait()

    def collect(v, l, side):
        hop(v, z, l, side, z).wait_recv()
        own[v, z, l] += p_in[v, side, z, l].astype(jnp.float32)

    def forward(v, a, l, side, to):
        hop(v, a, l, side, to).wait_recv()
        part[v, a, l] = (own[v, a, l] + p_in[v, side, a, l].astype(jnp.float32)).astype(jnp.bfloat16)
        hop(v, a, l, side, to).start()

    def way(v):
        return remote(y_out.at[v], y_in.at[v], y_send.at[v], y_recv.at[v], {"gz": other})

    def trade(v):
        y_out[v] = own[v, z, other].astype(jnp.bfloat16)
        way(v).start()

    def finish(v):
        mine = own[v, z, g].astype(jnp.bfloat16).astype(jnp.float32)
        way(v).wait_recv()
        theirs = y_in[v].astype(jnp.float32)
        for f in range(FRB):
            lines = slice(f * width, (f + 1) * width)
            here = (rm_ref[v] == f).astype(jnp.float32)
            there = (rm_in[v] == f).astype(jnp.float32)
            total = here * mine + there * theirs
            out_ref[v, lines, :] = (front_ref[v, lines, :].astype(jnp.float32) - total).astype(
                out_ref.dtype
            )


    def ahead(v, a, l):
        forward(v, a, l, inward, across_mid)

    def back(v, l):
        forward(v, near_end, l, outward, near_end)

    near, mid, end = next_in, last - next_in, last - z
    early = {0: ((near, other),), 1: ((mid, other), (mid, g)), 2: ((end, other), (end, g))}

    def edge_step(k):
        for a, l in early.get(k, ()):
            send(0, a, l)
        if k == 2 * count - 1:
            for a, l in ((end, other), (mid, other), (end, g), (near, other), (mid, g)):
                send(1, a, l)
            send(0, near, g)
            send(1, near, g)

    def shared_step(k):
        if k == 0:
            pl.when(inner)(lambda: launch(1))
            gather(1)
            gather(2)
        if k == 1:
            pl.when(inner)(lambda: carry_on(1))
        if k == 2:
            gather(3)
        if k == 3:
            for n in range(4, levels * rows):
                gather(n)

    def inner_step(k):
        if k == 3:
            ahead(0, across_mid, other)
            ahead(0, across_mid, g)
        if k == 4:
            ahead(0, far_end, other)
        if k == 5:
            ahead(0, far_end, g)
            back(0, other)
            ahead(1, far_end, other)
            back(0, g)
        if k == 6:
            collect(0, other, inward)
            collect(0, other, outward)
            trade(0)
            ahead(1, across_mid, other)
            back(1, other)
            collect(0, g, outward)
            ahead(1, far_end, g)
        if k == 7:
            collect(1, other, outward)
            collect(1, other, inward)
            trade(1)
            back(1, g)
            ahead(1, across_mid, g)
            collect(0, g, inward)
            finish(0)
            collect(1, g, outward)
            collect(1, g, inward)

    def body(k, carry):
        take(k)
        item(k)
        for step in range(levels * rows):
            @pl.when(k == step)
            def _(step=step):
                pl.when(at_end)(lambda: edge_step(step))
                shared_step(step)
                pl.when(inner)(lambda: inner_step(step))

        return carry

    lax.fori_loop(0, levels * rows, body, 0)

    @pl.when(at_end)
    def _():
        collect(0, other, outward)
        trade(0)
        collect(0, g, outward)
        collect(1, other, outward)
        trade(1)
        finish(0)
        collect(1, g, outward)

    finish(1)

    for copy in live_out:
        copy.wait_send()
    for v in range(levels):
        way(v).wait_send()
        pl.when(via_here)(cross(v).wait_send)
        pl.when(via_far)(onward(v).wait_send)
        pl.when(away)(place(v, 0).wait_send)
        pl.when(straight)(place(v, 1).wait_send)

        def drain(a, carry, v=v):
            turned = via(a, z)

            @pl.when(gate)
            def _():
                for h in range(2):
                    passes(v, a, h)[1].wait_send()

            pl.when(entry)(lambda: passes(v, a, 0)[0].wait_send())
            posted = jnp.logical_or(
                jnp.logical_and(entry, jnp.logical_not(turned)), jnp.logical_and(second, turned)
            )
            pl.when(posted)(lambda: passes(v, a, 1)[0].wait_send())

            @pl.when(a != z)
            def _():
                for l in range(layers):
                    hop(v, a, l, 0, z).wait_send()

            return carry

        lax.fori_loop(0, rows, drain, 0)


def stationary(rows, cols, layers, lpanel, upanel, rowmap, colmap, blockmask, front_blocks):
    levels, _, width, depth = lpanel.shape
    bf16 = jnp.bfloat16
    vmem = pl.BlockSpec(memory_space=pltpu.VMEM)
    hbm = pl.BlockSpec(memory_space=pl.ANY)
    dma = pltpu.SemaphoreType.DMA
    return pl.pallas_call(
        functools.partial(kernel, rows, cols, layers, levels, width),
        out_shape=jax.ShapeDtypeStruct(front_blocks.shape, front_blocks.dtype),
        in_specs=[hbm, hbm, vmem, vmem, vmem, hbm],
        out_specs=vmem,
        scratch_shapes=[
            pltpu.VMEM((levels, width, depth), bf16),
            pltpu.VMEM(upanel[:, 0].shape, bf16),
            pltpu.VMEM(front_blocks.shape, bf16),
            pltpu.VMEM((levels, width // 2, depth), bf16),
            pltpu.VMEM((levels, rows, width, depth), bf16),
            pltpu.VMEM((rows,) + blockmask.shape[:1] + blockmask.shape[2:], jnp.int32),
            pltpu.VMEM((levels, rows, layers, width, width), jnp.float32),
            pltpu.VMEM((levels, rows, layers, width, width), bf16),
            pltpu.VMEM((levels, 2, rows, layers, width, width), bf16),
            pltpu.VMEM((levels, width, width), bf16),
            pltpu.VMEM((levels, width, width), bf16),
            pltpu.VMEM(rowmap.shape, jnp.int32),
            dma((3,)),
            dma((levels,)),
            dma((levels,)),
            dma((levels,)),
            dma((levels,)),
            dma((levels, 2)),
            dma((levels, 2, rows)),
            dma((levels, 2, rows)),
            dma((levels, 2, rows)),
            dma((rows,)),
            dma((rows,)),
            dma,
            dma((levels, rows, layers)),
            dma((levels, 2, rows, layers)),
            dma((levels,)),
            dma((levels,)),
            dma,
            dma,
        ],
        compiler_params=pltpu.CompilerParams(collective_id=0, has_side_effects=True),
    )(lpanel[:, 0], upanel[:, 0], colmap, blockmask[:, 0], rowmap, front_blocks)


def solution(mesh):
    rows, cols, layers = mesh.shape["row"], mesh.shape["col"], mesh.shape["gz"]
    body = general
    if rows == cols == 2 * layers and layers == 2:
        body = functools.partial(stationary, rows, cols, layers)
    return jax.shard_map(
        body,
        mesh=mesh,
        in_specs=(
            P(None, "gz", "row", "col"),
            P(None, "gz", "row", "col"),
            P(None, "gz", "row"),
            P(None, "gz", "col"),
            P(None, "gz", "row", "col"),
            P(None, "row", ("gz", "col")),
        ),
        out_specs=P(None, "row", ("gz", "col")),
        check_vma=False,
    )
```

```python
import functools

import jax
import jax.numpy as jnp
from jax import lax
from jax.experimental import pallas as pl
from jax.experimental.pallas import tpu as pltpu
from jax.sharding import PartitionSpec as P

CB = 4
FRB = 2
MESH = pl.DeviceIdType.MESH


def column_sums(schur, cols_of, live, layers):
    width = schur.shape[0]
    blocks = schur.reshape(width, CB, width)
    targets = cols_of[:, None] == jnp.arange(layers, dtype=jnp.int32)[None, :]
    col_select = targets.astype(jnp.float32) * live.astype(jnp.float32)[:, None]
    return jnp.einsum("bjk,jl->lbk", blocks, col_select, precision=lax.Precision.HIGHEST)


def general(lpanel, upanel, rowmap, colmap, blockmask, front_blocks):
    layers = lax.axis_size("gz")
    width = lpanel.shape[2]
    levels = lpanel.shape[0]
    tiles = []
    for depth in range(levels):
        left_rows = lax.all_gather(lpanel[depth, 0], "col", axis=1, tiled=True)
        tiles.append(
            jnp.dot(
                left_rows,
                lax.all_gather(upanel[depth, 0], "row", axis=0, tiled=True),
                preferred_element_type=jnp.float32,
            )
        )
    results = []
    every_row = lax.all_gather(rowmap[:, :, 0], "gz", axis=1, tiled=True)
    for depth in range(levels):
        sums = column_sums(tiles[depth], colmap[depth, 0], blockmask[depth, 0, 0], layers).astype(
            jnp.bfloat16
        )
        arrived = lax.all_to_all(sums, "gz", split_axis=0, concat_axis=0, tiled=True)
        row_select = (
            every_row[depth][:, None] == jnp.arange(FRB, dtype=jnp.int32)[None, :]
        ).astype(jnp.float32)
        placed = jnp.einsum(
            "sf,sbk->fbk", row_select, arrived.astype(jnp.float32), precision=lax.Precision.HIGHEST
        )
        placed = placed.reshape(FRB * width, width)
        results.append((front_blocks[depth].astype(jnp.float32) - placed).astype(jnp.bfloat16))
    return jnp.stack(results)


def kernel(
    rows, cols, layers, levels, width,
    l_hbm, u_hbm, cm_hbm, live_hbm, rm_hbm, front_hbm, out_ref,
    cm_ref, live_ref, rm_ref,
    l_ref, u_ref, front_ref, crossed, l_all, live_all, own, part, p_in, y_out, y_in, rm_in,
    in_sem, own_sem, x_send, x_recv, c_send, l_send, l_recv, post_send, relay_send,
    m_send, m_recv, p_send, p_recv, y_send, y_recv, rm_send, rm_recv,
):
    z = lax.axis_index("row")
    c = lax.axis_index("col")
    g = lax.axis_index("gz")
    far = lax.rem(c + cols // 2, cols)
    mate = c + 1 - 2 * lax.rem(c, 2)
    other = 1 - g
    last = rows - 1
    entry, second = c == z, far == z
    gate = jnp.logical_or(entry, second)
    low = 1 - z // (rows // 2)
    depth = low * z + (1 - low) * (last - z)
    at_end = depth == 0
    inner = jnp.logical_not(at_end)

    def remote(src, dst, send, recv, where):
        return pltpu.make_async_remote_copy(
            src_ref=src, dst_ref=dst, send_sem=send, recv_sem=recv,
            device_id=where, device_id_type=MESH,
        )

    barrier = pltpu.get_barrier_semaphore()
    for step in range(1, rows):
        pl.semaphore_signal(
            barrier, inc=1, device_id={"row": lax.rem(z + step, rows)}, device_id_type=MESH
        )
    pl.semaphore_signal(barrier, inc=1, device_id={"col": far}, device_id_type=MESH)
    pl.semaphore_signal(barrier, inc=1, device_id={"col": mate}, device_id_type=MESH)
    pl.semaphore_signal(barrier, inc=1, device_id={"gz": other}, device_id_type=MESH)

    first = pltpu.make_async_copy(l_hbm, l_ref, in_sem.at[0])
    first.start()
    small = [
        pltpu.make_async_copy(src, dst, in_sem.at[3 + i])
        for i, (src, dst) in enumerate(
            ((live_hbm, live_ref), (rm_hbm, rm_ref), (cm_hbm, cm_ref), (live_hbm, live_all.at[z]))
        )
    ]
    for copy in small:
        copy.start()
    whole_u = pltpu.make_async_copy(u_hbm, u_ref, in_sem.at[1])
    whole_u.start()
    fronts = pltpu.make_async_copy(front_hbm, front_ref, in_sem.at[2])
    fronts.start()

    def own_load(v):
        return pltpu.make_async_copy(l_hbm.at[v], l_all.at[v, z], own_sem.at[v])

    @pl.when(entry)
    def _():
        for v in range(levels):
            own_load(v).start()

    for copy in small:
        copy.wait()
    first.wait()
    pl.semaphore_wait(barrier, rows + 2)

    half = width // 2
    pieces = [slice(h * half, (h + 1) * half) for h in range(2)]

    def short(r, q):
        return jnp.logical_and(r * (last - r) > 0, q * (last - q) == 0)

    def place(v, h):
        return remote(
            l_ref.at[v, pieces[h]], l_all.at[v, z, pieces[h]],
            l_send.at[v, h], l_recv.at[v, h, z], {"row": c},
        )

    def cross(v):
        return remote(
            l_ref.at[v, pieces[1]], crossed.at[v], x_send.at[v], x_recv.at[v], {"col": far}
        )

    def onward(v):
        return remote(
            crossed.at[v], l_all.at[v, z, pieces[1]], c_send.at[v], l_recv.at[v, 1, z], {"row": far}
        )

    away, helper = jnp.logical_not(entry), jnp.logical_not(second)
    direct, helps_direct = short(z, c), short(z, far)
    crosses = [jnp.logical_and(away, jnp.logical_not(direct)), away]
    helps = [jnp.logical_and(helper, jnp.logical_not(helps_direct)), helper]

    def launch(v):
        place(v, 0).start()
        pl.when(crosses[v])(lambda: cross(v).start())
        if v == 0:
            pl.when(direct)(lambda: place(v, 1).start())

    def carry_on(v):
        @pl.when(helps[v])
        def _():
            cross(v).wait_recv()
            onward(v).start()

    live_out = []
    for step in range(1, rows):
        to = lax.rem(z + step, rows)
        live_out.append(
            remote(live_ref, live_all.at[z], m_send.at[step], m_recv.at[z], {"row": to})
        )
        live_out[-1].start()
    rm_copy = remote(rm_ref, rm_in, rm_send, rm_recv, {"gz": other})
    rm_copy.start()
    gap = (z - c) * (z - c)
    beside = gap == 1
    patient = jnp.logical_and(gap >= 4, c * (last - c) == 0)
    eager = jnp.logical_and(away, jnp.logical_not(patient))
    lead = jnp.logical_and(beside, jnp.logical_or(at_end, direct))
    outer_two = jnp.logical_and(at_end, gap == 4)
    outer_three = gap == 9
    later = jnp.logical_and(inner, jnp.logical_and(away, jnp.logical_not(lead)))
    pl.when(eager)(lambda: launch(0))
    pl.when(lead)(lambda: launch(1))

    def passes(v, a, h):
        spot = l_all.at[v, a, pieces[h]]
        post = remote(spot, spot, post_send.at[v, h, a], l_recv.at[v, h, a], {"col": far})
        relay = remote(spot, spot, relay_send.at[v, h, a], l_recv.at[v, h, a], {"col": mate})
        return post, relay

    count = rows - 1

    def place_of(k):
        mine = k // (levels * count)
        first = 1 - (k + levels) // (2 * levels)
        rest = k - levels
        v = first * k + (1 - first) * (rest // levels)
        step = lax.rem(rest + 2 * levels, levels)
        i = (1 - first) * (1 + step + v * (1 - 2 * step))
        near = (1 - depth) * (i + 1) + depth * (i + (i + 1) // 2)
        near = low * near + (1 - low) * (last - near)
        v = mine * (k - levels * count) + (1 - mine) * v
        return v, mine * z + (1 - mine) * near

    def turned(v, a, h):
        if h == 0:
            return a < 0
        plain = jnp.logical_or(a == z, jnp.logical_and(v == 0, short(a, z)))
        return jnp.logical_not(plain)

    def spread(v, a, h):
        post, relay = passes(v, a, h)
        post.start()
        relay.start()

    def gather_entry(k):
        v, a = place_of(k)

        @pl.when(entry)
        def _():
            pl.when(a == z)(lambda: own_load(v).wait())
            for h in range(2):
                @pl.when(jnp.logical_not(turned(v, a, h)))
                def _(h=h):
                    pl.when(a != z)(lambda: passes(v, a, h)[1].wait_recv())
                    spread(v, a, h)

    def gather_second(k):
        v, a = place_of(k)
        for h in range(2):
            @pl.when(jnp.logical_and(second, turned(v, a, h)))
            def _(h=h):
                passes(v, a, h)[1].wait_recv()
                spread(v, a, h)

    def gather(k):
        gather_entry(k)
        gather_second(k)

    def take(k):
        v, a = place_of(k)

        def hand(h):
            relay = passes(v, a, h)[1]
            relay.wait_recv()
            relay.start()

        for h in range(2):
            there = turned(v, a, h)
            taken = jnp.logical_or(
                jnp.logical_and(second, jnp.logical_not(there)), jnp.logical_and(entry, there)
            )
            pl.when(taken)(lambda h=h: hand(h))

        @pl.when(jnp.logical_not(gate))
        def _():
            for h in range(2):
                passes(v, a, h)[1].wait_recv()

    def hop(v, a, l, side, to):
        return remote(
            part.at[v, a, l], p_in.at[v, side, a, l],
            p_send.at[v, a, l], p_recv.at[v, side, a, l], {"row": to},
        )

    inward, outward = 1 - low, low
    near_end, far_end = last * inward, last * low
    across_mid = last - z
    next_in = low + (1 - low) * (last - 1)

    def send(v, a, l):
        part[v, a, l] = own[v, a, l].astype(jnp.bfloat16)
        hop(v, a, l, inward, next_in).start()

    def item(k):
        v, a = place_of(k)
        block = l_all[v, a]
        to_layer = cm_ref[v]
        live = live_all[a, v]
        for j in range(CB):
            t = jnp.dot(
                block, u_ref[v, :, j * width : (j + 1) * width], preferred_element_type=jnp.float32
            )
            for l in range(layers):
                m = jnp.where(to_layer[:, j : j + 1] == l, live[:, j : j + 1], 0).astype(jnp.float32)
                if j == 0:
                    own[v, a, l] = t * m
                else:
                    own[v, a, l] += t * m


    def hear(src):
        remote(live_ref, live_all.at[src], m_send.at[1], m_recv.at[src], {"row": src}).wait_recv()

    spare = jnp.logical_not(gate)
    busy_inner = jnp.logical_and(inner, gate)
    busy_end = jnp.logical_and(at_end, gate)
    pl.when(inner)(lambda: carry_on(0))
    hear(place_of(0)[1])
    pl.when(patient)(lambda: launch(0))
    pl.when(outer_two)(lambda: launch(1))
    gather_entry(0)

    @pl.when(inner)
    def _():
        gather_second(0)
        gather(2)
        gather(1)

    @pl.when(at_end)
    def _():
        carry_on(0)
        gather_second(1)

    pl.when(later)(lambda: launch(1))
    pl.when(outer_three)(lambda: launch(1))
    pl.when(spare)(lambda: carry_on(1))
    whole_u.wait()
    rm_copy.wait()
    fronts.wait()

    def collect(v, l, side):
        hop(v, z, l, side, z).wait_recv()
        own[v, z, l] += p_in[v, side, z, l].astype(jnp.float32)

    def forward(v, a, l, side, to):
        hop(v, a, l, side, to).wait_recv()
        part[v, a, l] = (own[v, a, l] + p_in[v, side, a, l].astype(jnp.float32)).astype(jnp.bfloat16)
        hop(v, a, l, side, to).start()

    def way(v):
        return remote(y_out.at[v], y_in.at[v], y_send.at[v], y_recv.at[v], {"gz": other})

    def trade(v):
        y_out[v] = own[v, z, other].astype(jnp.bfloat16)
        way(v).start()

    def finish(v):
        mine = own[v, z, g].astype(jnp.bfloat16).astype(jnp.float32)
        way(v).wait_recv()
        theirs = y_in[v].astype(jnp.float32)
        for f in range(FRB):
            lines = slice(f * width, (f + 1) * width)
            here = (rm_ref[0, :, v : v + 1] == f).astype(jnp.float32)
            there = (rm_in[0, :, v : v + 1] == f).astype(jnp.float32)
            total = here * mine + there * theirs
            out_ref[v, lines, :] = (front_ref[v, lines, :].astype(jnp.float32) - total).astype(
                out_ref.dtype
            )


    def ahead(v, a, l):
        forward(v, a, l, inward, across_mid)

    def back(v, l):
        forward(v, near_end, l, outward, near_end)

    near, mid, end = next_in, last - next_in, last - z
    early = {
        0: ((0, near, other),),
        1: ((1, near, other),),
        2: ((0, mid, other),),
        3: ((0, end, other), (0, end, g)),
        4: ((1, end, other), (1, end, g)),
        5: ((1, mid, other), (0, mid, g), (1, mid, g), (0, near, g), (1, near, g)),
    }

    def edge_step(k):
        for v, a, l in early.get(k, ()):
            send(v, a, l)

    def edge_gather(k):
        if k == 0:
            pl.when(busy_end)(lambda: carry_on(1))
            gather_second(2)
            gather_entry(1)
            gather_entry(2)
        if k == 1:
            gather(3)
        if k == 2:
            gather_entry(4)
        if k == 3:
            gather_second(4)
            gather(5)
            gather_entry(6)
            gather_entry(7)

    def inner_gather(k):
        if k == 0:
            pl.when(busy_inner)(lambda: carry_on(1))
            gather(3)
        if k == 1:
            gather(4)
        if k == 2:
            gather(5)
        if k == 3:
            gather_entry(6)
            gather_entry(7)

    def shared_step(k):
        pl.when(at_end)(lambda: edge_gather(k))
        pl.when(inner)(lambda: inner_gather(k))
        if k in (1, 2):
            hear(place_of(k + 1)[1])

    def inner_step(k):
        if k == 3:
            ahead(0, across_mid, other)
            ahead(0, far_end, other)
        if k == 5:
            ahead(0, far_end, g)
            ahead(1, far_end, other)
            back(0, other)
        if k == 6:
            collect(0, other, inward)
            collect(0, other, outward)
            trade(0)
            ahead(1, far_end, g)
            back(0, g)
        if k == 7:
            ahead(1, across_mid, other)
            back(1, other)
            ahead(0, across_mid, g)
            back(1, g)
            collect(1, other, inward)
            collect(1, other, outward)
            trade(1)
            ahead(1, across_mid, g)
            collect(0, g, outward)
            collect(0, g, inward)
            finish(0)
            collect(1, g, outward)
            collect(1, g, inward)

    def body(k, carry):
        take(k)
        item(k)
        for step in range(levels * rows):
            @pl.when(k == step)
            def _(step=step):
                pl.when(at_end)(lambda: edge_step(step))
                shared_step(step)
                pl.when(inner)(lambda: inner_step(step))

        return carry

    lax.fori_loop(0, levels * rows, body, 0)

    @pl.when(at_end)
    def _():
        collect(0, other, outward)
        trade(0)
        collect(0, g, outward)
        collect(1, other, outward)
        trade(1)
        finish(0)
        collect(1, g, outward)

    finish(1)

    for copy in live_out:
        copy.wait_send()
    for v in range(levels):
        way(v).wait_send()
        pl.when(crosses[v])(cross(v).wait_send)
        pl.when(helps[v])(onward(v).wait_send)
        pl.when(away)(place(v, 0).wait_send)
        if v == 0:
            pl.when(direct)(place(v, 1).wait_send)

        def drain(a, carry, v=v):
            for h in range(2):
                post, relay = passes(v, a, h)
                pl.when(gate)(relay.wait_send)
                there = turned(v, a, h)
                posted = jnp.logical_or(
                    jnp.logical_and(entry, jnp.logical_not(there)), jnp.logical_and(second, there)
                )
                pl.when(posted)(post.wait_send)

            @pl.when(a != z)
            def _():
                for l in range(layers):
                    hop(v, a, l, 0, z).wait_send()

            return carry

        lax.fori_loop(0, rows, drain, 0)


def stationary(rows, cols, layers, lpanel, upanel, rowmap, colmap, blockmask, front_blocks):
    levels, _, width, depth = lpanel.shape
    bf16 = jnp.bfloat16
    vmem = pl.BlockSpec(memory_space=pltpu.VMEM)
    hbm = pl.BlockSpec(memory_space=pl.ANY)
    dma = pltpu.SemaphoreType.DMA
    return pl.pallas_call(
        functools.partial(kernel, rows, cols, layers, levels, width),
        out_shape=jax.ShapeDtypeStruct(front_blocks.shape, front_blocks.dtype),
        in_specs=[hbm] * 6,
        out_specs=vmem,
        scratch_shapes=[
            pltpu.VMEM(colmap.shape, jnp.int32),
            pltpu.VMEM((levels,) + blockmask.shape[2:], jnp.int32),
            pltpu.VMEM((1, 1, levels), jnp.int32),
            pltpu.VMEM((levels, width, depth), bf16),
            pltpu.VMEM(upanel[:, 0].shape, bf16),
            pltpu.VMEM(front_blocks.shape, bf16),
            pltpu.VMEM((levels, width // 2, depth), bf16),
            pltpu.VMEM((levels, rows, width, depth), bf16),
            pltpu.VMEM((rows,) + blockmask.shape[:1] + blockmask.shape[2:], jnp.int32),
            pltpu.VMEM((levels, rows, layers, width, width), jnp.float32),
            pltpu.VMEM((levels, rows, layers, width, width), bf16),
            pltpu.VMEM((levels, 2, rows, layers, width, width), bf16),
            pltpu.VMEM((levels, width, width), bf16),
            pltpu.VMEM((levels, width, width), bf16),
            pltpu.VMEM((1, 1, levels), jnp.int32),
            dma((7,)),
            dma((levels,)),
            dma((levels,)),
            dma((levels,)),
            dma((levels,)),
            dma((levels, 2)),
            dma((levels, 2, rows)),
            dma((levels, 2, rows)),
            dma((levels, 2, rows)),
            dma((rows,)),
            dma((rows,)),
            dma((levels, rows, layers)),
            dma((levels, 2, rows, layers)),
            dma((levels,)),
            dma((levels,)),
            dma,
            dma,
        ],
        compiler_params=pltpu.CompilerParams(collective_id=0, has_side_effects=True),
    )(
        lpanel[:, 0], upanel[:, 0], colmap, blockmask[:, 0], jnp.transpose(rowmap, (1, 2, 0)),
        front_blocks,
    )


def solution(mesh):
    rows, cols, layers = mesh.shape["row"], mesh.shape["col"], mesh.shape["gz"]
    body = general
    if rows == cols == 2 * layers and layers == 2:
        body = functools.partial(stationary, rows, cols, layers)
    return jax.shard_map(
        body,
        mesh=mesh,
        in_specs=(
            P(None, "gz", "row", "col"),
            P(None, "gz", "row", "col"),
            P(None, "gz", "row"),
            P(None, "gz", "col"),
            P(None, "gz", "row", "col"),
            P(None, "row", ("gz", "col")),
        ),
        out_specs=P(None, "row", ("gz", "col")),
        check_vma=False,
    )
```

```python
import functools

import jax
import jax.numpy as jnp
from jax import lax
from jax.experimental import pallas as pl
from jax.experimental.pallas import tpu as pltpu
from jax.sharding import PartitionSpec as P

CB = 4
FRB = 2
MESH = pl.DeviceIdType.MESH


def column_sums(schur, cols_of, live, layers):
    width = schur.shape[0]
    blocks = schur.reshape(width, CB, width)
    targets = cols_of[:, None] == jnp.arange(layers, dtype=jnp.int32)[None, :]
    col_select = targets.astype(jnp.float32) * live.astype(jnp.float32)[:, None]
    return jnp.einsum("bjk,jl->lbk", blocks, col_select, precision=lax.Precision.HIGHEST)


def general(lpanel, upanel, rowmap, colmap, blockmask, front_blocks):
    layers = lax.axis_size("gz")
    width = lpanel.shape[2]
    levels = lpanel.shape[0]
    tiles = []
    for depth in range(levels):
        left_rows = lax.all_gather(lpanel[depth, 0], "col", axis=1, tiled=True)
        tiles.append(
            jnp.dot(
                left_rows,
                lax.all_gather(upanel[depth, 0], "row", axis=0, tiled=True),
                preferred_element_type=jnp.float32,
            )
        )
    results = []
    every_row = lax.all_gather(rowmap[:, :, 0], "gz", axis=1, tiled=True)
    for depth in range(levels):
        sums = column_sums(tiles[depth], colmap[depth, 0], blockmask[depth, 0, 0], layers).astype(
            jnp.bfloat16
        )
        arrived = lax.all_to_all(sums, "gz", split_axis=0, concat_axis=0, tiled=True)
        row_select = (
            every_row[depth][:, None] == jnp.arange(FRB, dtype=jnp.int32)[None, :]
        ).astype(jnp.float32)
        placed = jnp.einsum(
            "sf,sbk->fbk", row_select, arrived.astype(jnp.float32), precision=lax.Precision.HIGHEST
        )
        placed = placed.reshape(FRB * width, width)
        results.append((front_blocks[depth].astype(jnp.float32) - placed).astype(jnp.bfloat16))
    return jnp.stack(results)


def kernel(
    rows, cols, layers, levels, width,
    l_hbm, u_hbm, cm_hbm, live_hbm, rm_hbm, front_hbm, out_ref,
    cm_ref, live_ref, rm_ref,
    l_ref, u_ref, front_ref, crossed, l_all, live_all, own, part, p_in, y_out, y_in, rm_in,
    in_sem, own_sem, x_send, x_recv, c_send, l_send, l_recv, post_send, relay_send,
    m_send, m_recv, p_send, p_recv, y_send, y_recv, rm_send, rm_recv,
    turn, stash, f_send, f_recv, g_send,
):
    z = lax.axis_index("row")
    c = lax.axis_index("col")
    g = lax.axis_index("gz")
    far = lax.rem(c + cols // 2, cols)
    mate = c + 1 - 2 * lax.rem(c, 2)
    other = 1 - g
    last = rows - 1
    entry, second = c == z, far == z
    gate = jnp.logical_or(entry, second)
    low = 1 - z // (rows // 2)
    depth = low * z + (1 - low) * (last - z)
    at_end = depth == 0
    inner = jnp.logical_not(at_end)

    def remote(src, dst, send, recv, where):
        return pltpu.make_async_remote_copy(
            src_ref=src, dst_ref=dst, send_sem=send, recv_sem=recv,
            device_id=where, device_id_type=MESH,
        )

    barrier = pltpu.get_barrier_semaphore()
    for step in range(1, rows):
        pl.semaphore_signal(
            barrier, inc=1, device_id={"row": lax.rem(z + step, rows)}, device_id_type=MESH
        )
    pl.semaphore_signal(barrier, inc=1, device_id={"col": far}, device_id_type=MESH)
    pl.semaphore_signal(barrier, inc=1, device_id={"col": mate}, device_id_type=MESH)
    pl.semaphore_signal(barrier, inc=1, device_id={"gz": other}, device_id_type=MESH)

    first = pltpu.make_async_copy(l_hbm, l_ref, in_sem.at[0])
    first.start()
    small = [
        pltpu.make_async_copy(src, dst, in_sem.at[3 + i])
        for i, (src, dst) in enumerate(
            ((live_hbm, live_ref), (rm_hbm, rm_ref), (cm_hbm, cm_ref), (live_hbm, live_all.at[z]))
        )
    ]
    for copy in small:
        copy.start()
    whole_u = pltpu.make_async_copy(u_hbm, u_ref, in_sem.at[1])
    whole_u.start()
    fronts = pltpu.make_async_copy(front_hbm, front_ref, in_sem.at[2])
    fronts.start()

    def own_load(v):
        return pltpu.make_async_copy(l_hbm.at[v], l_all.at[v, z], own_sem.at[v])

    @pl.when(entry)
    def _():
        for v in range(levels):
            own_load(v).start()

    for copy in small:
        copy.wait()
    first.wait()
    pl.semaphore_wait(barrier, rows + 2)

    half = width // 2
    pieces = [slice(h * half, (h + 1) * half) for h in range(2)]

    def place(v, h):
        return remote(
            l_ref.at[v, pieces[h]], l_all.at[v, z, pieces[h]],
            l_send.at[v, h], l_recv.at[v, h, z], {"row": c},
        )

    def cross(v, h):
        return remote(
            l_ref.at[v, pieces[h]], crossed.at[v, pieces[h]],
            x_send.at[v, h], x_recv.at[v, h], {"col": far},
        )

    def onward(v, h):
        return remote(
            crossed.at[v, pieces[h]], l_all.at[v, z, pieces[h]],
            c_send.at[v, h], l_recv.at[v, h, z], {"row": far},
        )

    def routes(q):
        central = q * (last - q) > 0
        both = jnp.logical_and(jnp.logical_and(inner, central), q != z)
        one = jnp.logical_and(jnp.logical_and(at_end, central), (q - z) * (q - z) == 4)
        return both, jnp.logical_or(both, one)

    away = jnp.logical_not(entry)
    crosses, helps = routes(c), routes(far)
    places = [jnp.logical_and(away, jnp.logical_not(flag)) for flag in crosses]

    def launch(v):
        for h in range(2):
            pl.when(places[h])(lambda h=h: place(v, h).start())
            pl.when(crosses[h])(lambda h=h: cross(v, h).start())

    def carry_on(v):
        for h in range(2):
            @pl.when(helps[h])
            def _(h=h):
                cross(v, h).wait_recv()
                onward(v, h).start()

    live_out = []
    for step in range(1, rows):
        to = lax.rem(z + step, rows)
        live_out.append(
            remote(live_ref, live_all.at[z], m_send.at[step], m_recv.at[z], {"row": to})
        )
        live_out[-1].start()
    rm_copy = remote(rm_ref, rm_in, rm_send, rm_recv, {"gz": other})
    rm_copy.start()
    gap = (z - c) * (z - c)
    to_end = c * (last - c) == 0
    distant = gap == 9
    late = jnp.logical_and(inner, jnp.logical_and(gap == 4, to_end))
    opener = jnp.logical_and(inner, jnp.logical_and(gap == 1, to_end))
    nearby = jnp.logical_and(away, jnp.logical_not(distant))
    lead = jnp.logical_and(nearby, jnp.logical_not(late))
    near_end, far_end = last * (1 - low), last * low
    next_in = low + (1 - low) * (last - 1)

    def deposit(v):
        return remote(l_ref.at[v], stash.at[v], f_send.at[v], f_recv.at[v], {"row": next_in})

    def pick_up(v, h):
        return remote(
            stash.at[v, pieces[h]], l_all.at[v, near_end, pieces[h]],
            g_send.at[v, h], l_recv.at[v, h, near_end], {"row": c},
        )

    @pl.when(distant)
    def _():
        for v in range(levels):
            deposit(v).start()

    @pl.when(lead)
    def _():
        for v in range(levels):
            launch(v)

    @pl.when(opener)
    def _():
        place(1, 0).wait_send()
        pl.semaphore_signal(turn, inc=1, device_id={"row": last - z}, device_id_type=MESH)

    @pl.when(late)
    def _():
        pl.semaphore_wait(turn, 1)
        launch(0)
        for v in range(levels):
            deposit(v).wait_recv()
            for h in range(2):
                pick_up(v, h).start()
        launch(1)

    def passes(v, a, h):
        spot = l_all.at[v, a, pieces[h]]
        post = remote(spot, spot, post_send.at[v, h, a], l_recv.at[v, h, a], {"col": far})
        relay = remote(spot, spot, relay_send.at[v, h, a], l_recv.at[v, h, a], {"col": mate})
        return post, relay

    count = rows - 1

    def place_of(k):
        mine = k // (levels * count)
        first = 1 - (k + levels) // (2 * levels)
        rest = k - levels
        v = first * k + (1 - first) * (rest // levels)
        step = lax.rem(rest + 2 * levels, levels)
        i = (1 - first) * (1 + step + v * (1 - 2 * step))
        near = (1 - depth) * (i + 1) + depth * (i + (i + 1) // 2)
        near = low * near + (1 - low) * (last - near)
        v = mine * (k - levels * count) + (1 - mine) * v
        return v, mine * z + (1 - mine) * near

    def turned(v, a, h):
        both = a == last - z
        return jnp.logical_and(inner, both if h == 0 else jnp.logical_or(both, (a - z) * (a - z) == 4))

    def spread(v, a, h):
        post, relay = passes(v, a, h)
        post.start()
        relay.start()

    def gather_entry(k):
        v, a = place_of(k)

        @pl.when(entry)
        def _():
            pl.when(a == z)(lambda: own_load(v).wait())
            for h in range(2):
                @pl.when(jnp.logical_not(turned(v, a, h)))
                def _(h=h):
                    pl.when(a != z)(lambda: passes(v, a, h)[1].wait_recv())
                    spread(v, a, h)

    def gather_second(k):
        v, a = place_of(k)
        for h in range(2):
            @pl.when(jnp.logical_and(second, turned(v, a, h)))
            def _(h=h):
                passes(v, a, h)[1].wait_recv()
                spread(v, a, h)

    def gather(k):
        gather_entry(k)
        gather_second(k)

    def take(k):
        v, a = place_of(k)

        def hand(h):
            relay = passes(v, a, h)[1]
            relay.wait_recv()
            relay.start()

        for h in range(2):
            there = turned(v, a, h)
            taken = jnp.logical_or(
                jnp.logical_and(second, jnp.logical_not(there)), jnp.logical_and(entry, there)
            )
            pl.when(taken)(lambda h=h: hand(h))

        @pl.when(jnp.logical_not(gate))
        def _():
            for h in range(2):
                passes(v, a, h)[1].wait_recv()

    def hop(v, a, l, side, to):
        return remote(
            part.at[v, a, l], p_in.at[v, side, a, l],
            p_send.at[v, a, l], p_recv.at[v, side, a, l], {"row": to},
        )

    inward, outward = 1 - low, low
    across_mid = last - z

    def send(v, a, l):
        part[v, a, l] = own[v, a, l].astype(jnp.bfloat16)
        hop(v, a, l, inward, next_in).start()

    def item(k):
        v, a = place_of(k)
        block = l_all[v, a]
        to_layer = cm_ref[v]
        live = live_all[a, v]
        for j in range(CB):
            t = jnp.dot(
                block, u_ref[v, :, j * width : (j + 1) * width], preferred_element_type=jnp.float32
            )
            for l in range(layers):
                m = jnp.where(to_layer[:, j : j + 1] == l, live[:, j : j + 1], 0).astype(jnp.float32)
                if j == 0:
                    own[v, a, l] = t * m
                else:
                    own[v, a, l] += t * m


    def hear(src):
        remote(live_ref, live_all.at[src], m_send.at[1], m_recv.at[src], {"row": src}).wait_recv()

    hear(place_of(0)[1])
    gather_entry(0)
    carry_on(0)

    @pl.when(inner)
    def _():
        gather_entry(1)
        carry_on(1)
        gather(2)

    whole_u.wait()
    rm_copy.wait()
    fronts.wait()

    def collect(v, l, side):
        hop(v, z, l, side, z).wait_recv()
        own[v, z, l] += p_in[v, side, z, l].astype(jnp.float32)

    def forward(v, a, l, side, to):
        hop(v, a, l, side, to).wait_recv()
        part[v, a, l] = (own[v, a, l] + p_in[v, side, a, l].astype(jnp.float32)).astype(jnp.bfloat16)
        hop(v, a, l, side, to).start()

    def way(v):
        return remote(y_out.at[v], y_in.at[v], y_send.at[v], y_recv.at[v], {"gz": other})

    def trade(v):
        y_out[v] = own[v, z, other].astype(jnp.bfloat16)
        way(v).start()

    def finish(v):
        mine = own[v, z, g].astype(jnp.bfloat16).astype(jnp.float32)
        way(v).wait_recv()
        theirs = y_in[v].astype(jnp.float32)
        for f in range(FRB):
            lines = slice(f * width, (f + 1) * width)
            here = (rm_ref[0, :, v : v + 1] == f).astype(jnp.float32)
            there = (rm_in[0, :, v : v + 1] == f).astype(jnp.float32)
            total = here * mine + there * theirs
            out_ref[v, lines, :] = (front_ref[v, lines, :].astype(jnp.float32) - total).astype(
                out_ref.dtype
            )


    def ahead(v, a, l):
        forward(v, a, l, inward, across_mid)

    def back(v, l):
        forward(v, near_end, l, outward, near_end)

    near, mid, end = next_in, last - next_in, last - z
    early = {
        0: ((0, near, other),),
        1: ((1, near, other),),
        2: ((0, mid, other),),
        3: ((0, end, other), (0, end, g)),
        4: ((1, end, other), (1, end, g)),
        5: ((1, mid, other), (0, mid, g), (1, mid, g), (0, near, g), (1, near, g)),
    }

    def edge_step(k):
        for v, a, l in early.get(k, ()):
            send(v, a, l)

    def edge_gather(k):
        if k < 5:
            gather_entry(k + 1)
        if k == 0:
            carry_on(1)
        if k == 5:
            gather_entry(6)
            gather_entry(7)

    def inner_gather(k):
        if k < 3:
            gather(k + 3)
        if k == 3:
            gather_entry(6)
            gather_entry(7)

    def shared_step(k):
        pl.when(at_end)(lambda: edge_gather(k))
        pl.when(inner)(lambda: inner_gather(k))
        if k in (1, 2):
            hear(place_of(k + 1)[1])

    def inner_step(k):
        if k == 3:
            ahead(0, across_mid, other)
            ahead(0, far_end, other)
        if k == 5:
            ahead(0, far_end, g)
            ahead(1, far_end, other)
            back(0, other)
        if k == 6:
            collect(0, other, inward)
            collect(0, other, outward)
            trade(0)
            ahead(1, far_end, g)
            back(0, g)
        if k == 7:
            ahead(1, across_mid, other)
            back(1, other)
            ahead(0, across_mid, g)
            back(1, g)
            collect(1, other, inward)
            collect(1, other, outward)
            trade(1)
            ahead(1, across_mid, g)
            collect(0, g, outward)
            collect(0, g, inward)
            finish(0)
            collect(1, g, outward)
            collect(1, g, inward)

    def body(k, carry):
        take(k)
        item(k)
        for step in range(levels * rows):
            @pl.when(k == step)
            def _(step=step):
                pl.when(at_end)(lambda: edge_step(step))
                shared_step(step)
                pl.when(inner)(lambda: inner_step(step))

        return carry

    lax.fori_loop(0, levels * rows, body, 0)

    @pl.when(at_end)
    def _():
        collect(0, other, outward)
        trade(0)
        collect(0, g, outward)
        collect(1, other, outward)
        trade(1)
        finish(0)
        collect(1, g, outward)

    finish(1)

    for copy in live_out:
        copy.wait_send()
    for v in range(levels):
        way(v).wait_send()
        pl.when(distant)(deposit(v).wait_send)
        for h in range(2):
            pl.when(crosses[h])(cross(v, h).wait_send)
            pl.when(helps[h])(onward(v, h).wait_send)
            pending = jnp.logical_and(places[h], jnp.logical_not(distant))
            if v == 1 and h == 0:
                pending = jnp.logical_and(pending, jnp.logical_not(opener))
            pl.when(late)(pick_up(v, h).wait_send)
            pl.when(pending)(place(v, h).wait_send)

        def drain(a, carry, v=v):
            for h in range(2):
                post, relay = passes(v, a, h)
                pl.when(gate)(relay.wait_send)
                there = turned(v, a, h)
                posted = jnp.logical_or(
                    jnp.logical_and(entry, jnp.logical_not(there)), jnp.logical_and(second, there)
                )
                pl.when(posted)(post.wait_send)

            @pl.when(a != z)
            def _():
                for l in range(layers):
                    hop(v, a, l, 0, z).wait_send()

            return carry

        lax.fori_loop(0, rows, drain, 0)


def stationary(rows, cols, layers, lpanel, upanel, rowmap, colmap, blockmask, front_blocks):
    levels, _, width, depth = lpanel.shape
    bf16 = jnp.bfloat16
    vmem = pl.BlockSpec(memory_space=pltpu.VMEM)
    hbm = pl.BlockSpec(memory_space=pl.ANY)
    dma = pltpu.SemaphoreType.DMA
    return pl.pallas_call(
        functools.partial(kernel, rows, cols, layers, levels, width),
        out_shape=jax.ShapeDtypeStruct(front_blocks.shape, front_blocks.dtype),
        in_specs=[hbm] * 6,
        out_specs=vmem,
        scratch_shapes=[
            pltpu.VMEM(colmap.shape, jnp.int32),
            pltpu.VMEM((levels,) + blockmask.shape[2:], jnp.int32),
            pltpu.VMEM((1, 1, levels), jnp.int32),
            pltpu.VMEM((levels, width, depth), bf16),
            pltpu.VMEM(upanel[:, 0].shape, bf16),
            pltpu.VMEM(front_blocks.shape, bf16),
            pltpu.VMEM((levels, width, depth), bf16),
            pltpu.VMEM((levels, rows, width, depth), bf16),
            pltpu.VMEM((rows,) + blockmask.shape[:1] + blockmask.shape[2:], jnp.int32),
            pltpu.VMEM((levels, rows, layers, width, width), jnp.float32),
            pltpu.VMEM((levels, rows, layers, width, width), bf16),
            pltpu.VMEM((levels, 2, rows, layers, width, width), bf16),
            pltpu.VMEM((levels, width, width), bf16),
            pltpu.VMEM((levels, width, width), bf16),
            pltpu.VMEM((1, 1, levels), jnp.int32),
            dma((7,)),
            dma((levels,)),
            dma((levels, 2)),
            dma((levels, 2)),
            dma((levels, 2)),
            dma((levels, 2)),
            dma((levels, 2, rows)),
            dma((levels, 2, rows)),
            dma((levels, 2, rows)),
            dma((rows,)),
            dma((rows,)),
            dma((levels, rows, layers)),
            dma((levels, 2, rows, layers)),
            dma((levels,)),
            dma((levels,)),
            dma,
            dma,
            pltpu.SemaphoreType.REGULAR,
            pltpu.VMEM((levels, width, depth), bf16),
            dma((levels,)),
            dma((levels,)),
            dma((levels, 2)),
        ],
        compiler_params=pltpu.CompilerParams(collective_id=0, has_side_effects=True),
    )(
        lpanel[:, 0], upanel[:, 0], colmap, blockmask[:, 0], jnp.transpose(rowmap, (1, 2, 0)),
        front_blocks,
    )


def solution(mesh):
    rows, cols, layers = mesh.shape["row"], mesh.shape["col"], mesh.shape["gz"]
    body = general
    if rows == cols == 2 * layers and layers == 2:
        body = functools.partial(stationary, rows, cols, layers)
    return jax.shard_map(
        body,
        mesh=mesh,
        in_specs=(
            P(None, "gz", "row", "col"),
            P(None, "gz", "row", "col"),
            P(None, "gz", "row"),
            P(None, "gz", "col"),
            P(None, "gz", "row", "col"),
            P(None, "row", ("gz", "col")),
        ),
        out_specs=P(None, "row", ("gz", "col")),
        check_vma=False,
    )
```

```python
import functools

import jax
import jax.numpy as jnp
from jax import lax
from jax.experimental import pallas as pl
from jax.experimental.pallas import tpu as pltpu
from jax.sharding import PartitionSpec as P

CB = 4
FRB = 2
MESH = pl.DeviceIdType.MESH


def column_sums(schur, cols_of, live, layers):
    width = schur.shape[0]
    blocks = schur.reshape(width, CB, width)
    targets = cols_of[:, None] == jnp.arange(layers, dtype=jnp.int32)[None, :]
    col_select = targets.astype(jnp.float32) * live.astype(jnp.float32)[:, None]
    return jnp.einsum("bjk,jl->lbk", blocks, col_select, precision=lax.Precision.HIGHEST)


def general(lpanel, upanel, rowmap, colmap, blockmask, front_blocks):
    layers = lax.axis_size("gz")
    width = lpanel.shape[2]
    levels = lpanel.shape[0]
    tiles = []
    for depth in range(levels):
        left_rows = lax.all_gather(lpanel[depth, 0], "col", axis=1, tiled=True)
        tiles.append(
            jnp.dot(
                left_rows,
                lax.all_gather(upanel[depth, 0], "row", axis=0, tiled=True),
                preferred_element_type=jnp.float32,
            )
        )
    results = []
    every_row = lax.all_gather(rowmap[:, :, 0], "gz", axis=1, tiled=True)
    for depth in range(levels):
        sums = column_sums(tiles[depth], colmap[depth, 0], blockmask[depth, 0, 0], layers).astype(
            jnp.bfloat16
        )
        arrived = lax.all_to_all(sums, "gz", split_axis=0, concat_axis=0, tiled=True)
        row_select = (
            every_row[depth][:, None] == jnp.arange(FRB, dtype=jnp.int32)[None, :]
        ).astype(jnp.float32)
        placed = jnp.einsum(
            "sf,sbk->fbk", row_select, arrived.astype(jnp.float32), precision=lax.Precision.HIGHEST
        )
        placed = placed.reshape(FRB * width, width)
        results.append((front_blocks[depth].astype(jnp.float32) - placed).astype(jnp.bfloat16))
    return jnp.stack(results)


def kernel(
    rows, cols, layers, levels, width,
    l_hbm, u_hbm, cm_hbm, live_hbm, rm_hbm, front_hbm, out_ref,
    cm_ref, live_ref, rm_ref,
    l_ref, u_ref, front_ref, crossed, l_all, live_all, own, part, p_in, y_out, y_in, rm_in,
    in_sem, own_sem, x_send, x_recv, c_send, l_send, l_recv, post_send, relay_send,
    m_send, m_recv, p_send, p_recv, y_send, y_recv, rm_send, rm_recv,
    turn, stash, f_send, f_recv, g_send,
):
    z = lax.axis_index("row")
    c = lax.axis_index("col")
    g = lax.axis_index("gz")
    far = lax.rem(c + cols // 2, cols)
    mate = c + 1 - 2 * lax.rem(c, 2)
    other = 1 - g
    last = rows - 1
    entry, second = c == z, far == z
    gate = jnp.logical_or(entry, second)
    low = 1 - z // (rows // 2)
    depth = low * z + (1 - low) * (last - z)
    at_end = depth == 0
    inner = jnp.logical_not(at_end)

    def remote(src, dst, send, recv, where):
        return pltpu.make_async_remote_copy(
            src_ref=src, dst_ref=dst, send_sem=send, recv_sem=recv,
            device_id=where, device_id_type=MESH,
        )

    barrier = pltpu.get_barrier_semaphore()
    for step in range(1, rows):
        pl.semaphore_signal(
            barrier, inc=1, device_id={"row": lax.rem(z + step, rows)}, device_id_type=MESH
        )
    pl.semaphore_signal(barrier, inc=1, device_id={"col": far}, device_id_type=MESH)
    pl.semaphore_signal(barrier, inc=1, device_id={"col": mate}, device_id_type=MESH)
    pl.semaphore_signal(barrier, inc=1, device_id={"gz": other}, device_id_type=MESH)

    first = pltpu.make_async_copy(l_hbm, l_ref, in_sem.at[0])
    first.start()
    small = [
        pltpu.make_async_copy(src, dst, in_sem.at[3 + i])
        for i, (src, dst) in enumerate(
            ((live_hbm, live_ref), (rm_hbm, rm_ref), (cm_hbm, cm_ref), (live_hbm, live_all.at[z]))
        )
    ]
    for copy in small:
        copy.start()
    whole_u = pltpu.make_async_copy(u_hbm, u_ref, in_sem.at[1])
    whole_u.start()
    fronts = pltpu.make_async_copy(front_hbm, front_ref, in_sem.at[2])
    fronts.start()

    def own_load(v):
        return pltpu.make_async_copy(l_hbm.at[v], l_all.at[v, z], own_sem.at[v])

    @pl.when(entry)
    def _():
        for v in range(levels):
            own_load(v).start()

    for copy in small:
        copy.wait()
    first.wait()
    pl.semaphore_wait(barrier, rows + 2)

    half = width // 2
    pieces = [slice(h * half, (h + 1) * half) for h in range(2)]

    def place(v, h):
        return remote(
            l_ref.at[v, pieces[h]], l_all.at[v, z, pieces[h]],
            l_send.at[v, h], l_recv.at[v, h, z], {"row": c},
        )

    def cross(v, h):
        return remote(
            l_ref.at[v, pieces[h]], crossed.at[v, pieces[h]],
            x_send.at[v, h], x_recv.at[v, h], {"col": far},
        )

    def onward(v, h):
        return remote(
            crossed.at[v, pieces[h]], l_all.at[v, z, pieces[h]],
            c_send.at[v, h], l_recv.at[v, h, z], {"row": far},
        )

    def routes(q):
        central = q * (last - q) > 0
        both = jnp.logical_and(jnp.logical_and(inner, central), q != z)
        one = jnp.logical_and(jnp.logical_and(at_end, central), (q - z) * (q - z) == 4)
        return both, jnp.logical_or(both, one)

    away = jnp.logical_not(entry)
    crosses, helps = routes(c), routes(far)
    places = [jnp.logical_and(away, jnp.logical_not(flag)) for flag in crosses]

    def launch(v):
        for h in range(2):
            pl.when(places[h])(lambda h=h: place(v, h).start())
            pl.when(crosses[h])(lambda h=h: cross(v, h).start())

    def carry_on(v):
        for h in range(2):
            @pl.when(helps[h])
            def _(h=h):
                cross(v, h).wait_recv()
                onward(v, h).start()

    live_out = []
    for step in range(1, rows):
        to = lax.rem(z + step, rows)
        live_out.append(
            remote(live_ref, live_all.at[z], m_send.at[step], m_recv.at[z], {"row": to})
        )
        live_out[-1].start()
    rm_copy = remote(rm_ref, rm_in, rm_send, rm_recv, {"gz": other})
    rm_copy.start()
    gap = (z - c) * (z - c)
    to_end = c * (last - c) == 0
    distant = gap == 9
    late = jnp.logical_and(inner, jnp.logical_and(gap == 4, to_end))
    opener = jnp.logical_and(inner, jnp.logical_and(gap == 1, to_end))
    nearby = jnp.logical_and(away, jnp.logical_not(distant))
    lead = jnp.logical_and(nearby, jnp.logical_not(late))
    near_end, far_end = last * (1 - low), last * low
    next_in = low + (1 - low) * (last - 1)

    def deposit(v):
        return remote(l_ref.at[v], stash.at[v], f_send.at[v], f_recv.at[v], {"row": next_in})

    def pick_up(v, h):
        return remote(
            stash.at[v, pieces[h]], l_all.at[v, near_end, pieces[h]],
            g_send.at[v, h], l_recv.at[v, h, near_end], {"row": c},
        )

    @pl.when(distant)
    def _():
        for v in range(levels):
            deposit(v).start()

    @pl.when(lead)
    def _():
        for v in range(levels):
            launch(v)

    @pl.when(opener)
    def _():
        place(1, 0).wait_send()
        pl.semaphore_signal(turn, inc=1, device_id={"row": last - z}, device_id_type=MESH)

    @pl.when(late)
    def _():
        pl.semaphore_wait(turn, 1)
        launch(0)
        for v in range(levels):
            deposit(v).wait_recv()
            for h in range(2):
                pick_up(v, h).start()
        launch(1)

    def passes(v, a, h):
        spot = l_all.at[v, a, pieces[h]]
        post = remote(spot, spot, post_send.at[v, h, a], l_recv.at[v, h, a], {"col": far})
        relay = remote(spot, spot, relay_send.at[v, h, a], l_recv.at[v, h, a], {"col": mate})
        return post, relay

    count = rows - 1

    def place_of(k):
        mine = k // (levels * count)
        first = 1 - (k + levels) // (2 * levels)
        rest = k - levels
        v = first * k + (1 - first) * (rest // levels)
        step = lax.rem(rest + 2 * levels, levels)
        i = (1 - first) * (1 + step + v * (1 - 2 * step))
        near = (1 - depth) * (i + 1) + depth * (i + (i + 1) // 2)
        near = low * near + (1 - low) * (last - near)
        v = mine * (k - levels * count) + (1 - mine) * v
        return v, mine * z + (1 - mine) * near

    def turned(v, a, h):
        both = a == last - z
        return jnp.logical_and(inner, both if h == 0 else jnp.logical_or(both, (a - z) * (a - z) == 4))

    def spread(v, a, h):
        post, relay = passes(v, a, h)
        post.start()
        relay.start()

    def gather_entry(k):
        v, a = place_of(k)

        @pl.when(entry)
        def _():
            pl.when(a == z)(lambda: own_load(v).wait())
            for h in range(2):
                @pl.when(jnp.logical_not(turned(v, a, h)))
                def _(h=h):
                    pl.when(a != z)(lambda: passes(v, a, h)[1].wait_recv())
                    spread(v, a, h)

    def gather_second(k):
        v, a = place_of(k)
        for h in range(2):
            @pl.when(jnp.logical_and(second, turned(v, a, h)))
            def _(h=h):
                passes(v, a, h)[1].wait_recv()
                spread(v, a, h)

    def gather(k):
        gather_entry(k)
        gather_second(k)

    def take(k):
        v, a = place_of(k)

        def hand(h):
            relay = passes(v, a, h)[1]
            relay.wait_recv()
            relay.start()

        for h in range(2):
            there = turned(v, a, h)
            taken = jnp.logical_or(
                jnp.logical_and(second, jnp.logical_not(there)), jnp.logical_and(entry, there)
            )
            pl.when(taken)(lambda h=h: hand(h))

        @pl.when(jnp.logical_not(gate))
        def _():
            for h in range(2):
                passes(v, a, h)[1].wait_recv()

    def hop(v, a, l, side, to):
        return remote(
            part.at[v, a, l], p_in.at[v, side, a, l],
            p_send.at[v, a, l], p_recv.at[v, side, a, l], {"row": to},
        )

    inward, outward = 1 - low, low
    across_mid = last - z

    def send(v, a, l):
        part[v, a, l] = own[v, a, l].astype(jnp.bfloat16)
        hop(v, a, l, inward, next_in).start()

    def item(k):
        v, a = place_of(k)
        block = l_all[v, a]
        to_layer = cm_ref[v]
        live = live_all[a, v]
        for j in range(CB):
            t = jnp.dot(
                block, u_ref[v, :, j * width : (j + 1) * width], preferred_element_type=jnp.float32
            )
            for l in range(layers):
                m = jnp.where(to_layer[:, j : j + 1] == l, live[:, j : j + 1], 0).astype(jnp.float32)
                if j == 0:
                    own[v, a, l] = t * m
                else:
                    own[v, a, l] += t * m


    def hear(src):
        remote(live_ref, live_all.at[src], m_send.at[1], m_recv.at[src], {"row": src}).wait_recv()

    hear(place_of(0)[1])
    gather_entry(0)
    carry_on(0)

    @pl.when(inner)
    def _():
        gather_entry(1)
        carry_on(1)
        gather(2)

    whole_u.wait()
    rm_copy.wait()
    fronts.wait()

    def collect(v, l, side):
        hop(v, z, l, side, z).wait_recv()
        own[v, z, l] += p_in[v, side, z, l].astype(jnp.float32)

    def forward(v, a, l, side, to):
        hop(v, a, l, side, to).wait_recv()
        part[v, a, l] = (own[v, a, l] + p_in[v, side, a, l].astype(jnp.float32)).astype(jnp.bfloat16)
        hop(v, a, l, side, to).start()

    def way(v):
        return remote(y_out.at[v], y_in.at[v], y_send.at[v], y_recv.at[v], {"gz": other})

    def trade(v):
        y_out[v] = own[v, z, other].astype(jnp.bfloat16)
        way(v).start()

    def finish(v):
        mine = own[v, z, g].astype(jnp.bfloat16).astype(jnp.float32)
        way(v).wait_recv()
        theirs = y_in[v].astype(jnp.float32)
        for f in range(FRB):
            lines = slice(f * width, (f + 1) * width)
            here = (rm_ref[0, :, v : v + 1] == f).astype(jnp.float32)
            there = (rm_in[0, :, v : v + 1] == f).astype(jnp.float32)
            total = here * mine + there * theirs
            out_ref[v, lines, :] = (front_ref[v, lines, :].astype(jnp.float32) - total).astype(
                out_ref.dtype
            )


    def ahead(v, a, l):
        forward(v, a, l, inward, across_mid)

    def back(v, l):
        forward(v, near_end, l, outward, near_end)

    near, mid, end = next_in, last - next_in, last - z
    early = {
        0: ((0, near, other),),
        1: ((1, near, other),),
        2: ((0, mid, other),),
        3: ((0, end, other),),
        4: ((1, end, other), (0, end, g), (1, end, g)),
        5: ((1, mid, other), (0, mid, g), (1, mid, g), (0, near, g), (1, near, g)),
    }

    def edge_step(k):
        for v, a, l in early.get(k, ()):
            send(v, a, l)

    def edge_gather(k):
        if k < 5:
            gather_entry(k + 1)
        if k == 0:
            carry_on(1)
        if k == 5:
            gather_entry(6)
            gather_entry(7)

    def inner_gather(k):
        if k < 3:
            gather(k + 3)
        if k == 3:
            gather_entry(6)
            gather_entry(7)

    def shared_step(k):
        pl.when(at_end)(lambda: edge_gather(k))
        pl.when(inner)(lambda: inner_gather(k))
        if k in (1, 2):
            hear(place_of(k + 1)[1])

    def hops_out(v):
        for step in range(1, rows):
            a = lax.rem(z + step, rows)
            for l in range(layers):
                hop(v, a, l, 0, a).wait_send()

    def settle():
        for copy in live_out:
            copy.wait_send()
        for v in range(levels):
            pl.when(distant)(deposit(v).wait_send)
            for h in range(2):
                pl.when(crosses[h])(cross(v, h).wait_send)
                pl.when(helps[h])(onward(v, h).wait_send)
                pending = jnp.logical_and(places[h], jnp.logical_not(distant))
                if v == 1 and h == 0:
                    pending = jnp.logical_and(pending, jnp.logical_not(opener))
                pl.when(late)(pick_up(v, h).wait_send)
                pl.when(pending)(place(v, h).wait_send)

        @pl.when(gate)
        def _():
            for v in range(levels):
                def drain(a, carry, v=v):
                    for h in range(2):
                        post, relay = passes(v, a, h)
                        relay.wait_send()
                        there = turned(v, a, h)
                        posted = jnp.logical_or(
                            jnp.logical_and(entry, jnp.logical_not(there)),
                            jnp.logical_and(second, there),
                        )
                        pl.when(posted)(post.wait_send)
                    return carry

                lax.fori_loop(0, rows, drain, 0)

        for v in range(levels - 1):
            way(v).wait_send()
            hops_out(v)

    def inner_step(k):
        if k == 3:
            ahead(0, across_mid, other)
            ahead(0, far_end, other)
        if k == 5:
            ahead(1, far_end, other)
            ahead(0, far_end, g)
            back(0, other)
        if k == 6:
            collect(0, other, inward)
            collect(0, other, outward)
            trade(0)
            ahead(1, far_end, g)
            back(1, other)
        if k == 7:
            ahead(1, across_mid, other)
            back(0, g)
            ahead(0, across_mid, g)
            back(1, g)
            collect(1, other, inward)
            collect(1, other, outward)
            trade(1)
            ahead(1, across_mid, g)
            settle()
            collect(0, g, outward)
            collect(0, g, inward)
            finish(0)
            collect(1, g, outward)
            collect(1, g, inward)

    def body(k, carry):
        take(k)
        item(k)
        for step in range(levels * rows):
            @pl.when(k == step)
            def _(step=step):
                pl.when(at_end)(lambda: edge_step(step))
                shared_step(step)
                pl.when(inner)(lambda: inner_step(step))

        return carry

    lax.fori_loop(0, levels * rows, body, 0)

    @pl.when(at_end)
    def _():
        collect(0, other, outward)
        trade(0)
        collect(1, other, outward)
        trade(1)
        collect(0, g, outward)
        settle()
        finish(0)
        collect(1, g, outward)

    finish(1)
    hops_out(levels - 1)
    way(levels - 1).wait_send()


def stationary(rows, cols, layers, lpanel, upanel, rowmap, colmap, blockmask, front_blocks):
    levels, _, width, depth = lpanel.shape
    bf16 = jnp.bfloat16
    vmem = pl.BlockSpec(memory_space=pltpu.VMEM)
    hbm = pl.BlockSpec(memory_space=pl.ANY)
    dma = pltpu.SemaphoreType.DMA
    return pl.pallas_call(
        functools.partial(kernel, rows, cols, layers, levels, width),
        out_shape=pltpu.VMEM(front_blocks.shape, front_blocks.dtype),
        in_specs=[hbm] * 6,
        out_specs=vmem,
        scratch_shapes=[
            pltpu.VMEM(colmap.shape, jnp.int32),
            pltpu.VMEM((levels,) + blockmask.shape[2:], jnp.int32),
            pltpu.VMEM((1, 1, levels), jnp.int32),
            pltpu.VMEM((levels, width, depth), bf16),
            pltpu.VMEM(upanel[:, 0].shape, bf16),
            pltpu.VMEM(front_blocks.shape, bf16),
            pltpu.VMEM((levels, width, depth), bf16),
            pltpu.VMEM((levels, rows, width, depth), bf16),
            pltpu.VMEM((rows,) + blockmask.shape[:1] + blockmask.shape[2:], jnp.int32),
            pltpu.VMEM((levels, rows, layers, width, width), jnp.float32),
            pltpu.VMEM((levels, rows, layers, width, width), bf16),
            pltpu.VMEM((levels, 2, rows, layers, width, width), bf16),
            pltpu.VMEM((levels, width, width), bf16),
            pltpu.VMEM((levels, width, width), bf16),
            pltpu.VMEM((1, 1, levels), jnp.int32),
            dma((7,)),
            dma((levels,)),
            dma((levels, 2)),
            dma((levels, 2)),
            dma((levels, 2)),
            dma((levels, 2)),
            dma((levels, 2, rows)),
            dma((levels, 2, rows)),
            dma((levels, 2, rows)),
            dma((rows,)),
            dma((rows,)),
            dma((levels, rows, layers)),
            dma((levels, 2, rows, layers)),
            dma((levels,)),
            dma((levels,)),
            dma,
            dma,
            pltpu.SemaphoreType.REGULAR,
            pltpu.VMEM((levels, width, depth), bf16),
            dma((levels,)),
            dma((levels,)),
            dma((levels, 2)),
        ],
        compiler_params=pltpu.CompilerParams(collective_id=0, has_side_effects=True),
    )(
        lpanel[:, 0], upanel[:, 0], colmap, blockmask[:, 0], jnp.transpose(rowmap, (1, 2, 0)),
        front_blocks,
    )


def solution(mesh):
    rows, cols, layers = mesh.shape["row"], mesh.shape["col"], mesh.shape["gz"]
    body = general
    if rows == cols == 2 * layers and layers == 2:
        body = functools.partial(stationary, rows, cols, layers)
    return jax.shard_map(
        body,
        mesh=mesh,
        in_specs=(
            P(None, "gz", "row", "col"),
            P(None, "gz", "row", "col"),
            P(None, "gz", "row"),
            P(None, "gz", "col"),
            P(None, "gz", "row", "col"),
            P(None, "row", ("gz", "col")),
        ),
        out_specs=P(None, "row", ("gz", "col")),
        check_vma=False,
    )
```

```python
import functools

import jax
import jax.numpy as jnp
from jax import lax
from jax.experimental import pallas as pl
from jax.experimental.pallas import tpu as pltpu
from jax.sharding import PartitionSpec as P

CB = 4
FRB = 2
MESH = pl.DeviceIdType.MESH


def column_sums(schur, cols_of, live, layers):
    width = schur.shape[0]
    blocks = schur.reshape(width, CB, width)
    targets = cols_of[:, None] == jnp.arange(layers, dtype=jnp.int32)[None, :]
    col_select = targets.astype(jnp.float32) * live.astype(jnp.float32)[:, None]
    return jnp.einsum("bjk,jl->lbk", blocks, col_select, precision=lax.Precision.HIGHEST)


def general(lpanel, upanel, rowmap, colmap, blockmask, front_blocks):
    layers = lax.axis_size("gz")
    width = lpanel.shape[2]
    levels = lpanel.shape[0]
    tiles = []
    for depth in range(levels):
        left_rows = lax.all_gather(lpanel[depth, 0], "col", axis=1, tiled=True)
        tiles.append(
            jnp.dot(
                left_rows,
                lax.all_gather(upanel[depth, 0], "row", axis=0, tiled=True),
                preferred_element_type=jnp.float32,
            )
        )
    results = []
    every_row = lax.all_gather(rowmap[:, :, 0], "gz", axis=1, tiled=True)
    for depth in range(levels):
        sums = column_sums(tiles[depth], colmap[depth, 0], blockmask[depth, 0, 0], layers).astype(
            jnp.bfloat16
        )
        arrived = lax.all_to_all(sums, "gz", split_axis=0, concat_axis=0, tiled=True)
        row_select = (
            every_row[depth][:, None] == jnp.arange(FRB, dtype=jnp.int32)[None, :]
        ).astype(jnp.float32)
        placed = jnp.einsum(
            "sf,sbk->fbk", row_select, arrived.astype(jnp.float32), precision=lax.Precision.HIGHEST
        )
        placed = placed.reshape(FRB * width, width)
        results.append((front_blocks[depth].astype(jnp.float32) - placed).astype(jnp.bfloat16))
    return jnp.stack(results)


def kernel(
    rows, cols, layers, levels, width,
    l_hbm, u_hbm, cm_hbm, live_hbm, rm_hbm, front_hbm, out_ref,
    cm_ref, rm_ref,
    l_ref, u_ref, front_ref, crossed, stash, l_all, live_all, own, part, p_in, y_out, y_in, rm_in,
    in_sem, own_sem, x_recv, c_send, l_send, l_recv, post_send, relay_send,
    m_send, m_recv, p_send, p_recv, y_send, y_recv, rm_send, rm_recv, turn, f_recv, g_send,
):
    z = lax.axis_index("row")
    c = lax.axis_index("col")
    g = lax.axis_index("gz")
    far = lax.rem(c + cols // 2, cols)
    mate = c + 1 - 2 * lax.rem(c, 2)
    other = 1 - g
    last = rows - 1
    entry, second = c == z, far == z
    gate = jnp.logical_or(entry, second)
    low = 1 - z // (rows // 2)
    depth = low * z + (1 - low) * (last - z)
    at_end = depth == 0
    inner = jnp.logical_not(at_end)

    def remote(src, dst, send, recv, where):
        return pltpu.make_async_remote_copy(
            src_ref=src, dst_ref=dst, send_sem=send, recv_sem=recv,
            device_id=where, device_id_type=MESH,
        )

    barrier = pltpu.get_barrier_semaphore()
    for step in range(1, rows):
        pl.semaphore_signal(
            barrier, inc=1, device_id={"row": lax.rem(z + step, rows)}, device_id_type=MESH
        )
    pl.semaphore_signal(barrier, inc=1, device_id={"col": far}, device_id_type=MESH)
    pl.semaphore_signal(barrier, inc=1, device_id={"col": mate}, device_id_type=MESH)
    pl.semaphore_signal(barrier, inc=1, device_id={"gz": other}, device_id_type=MESH)

    first = pltpu.make_async_copy(l_hbm, l_ref, in_sem.at[0])
    first.start()
    small = [
        pltpu.make_async_copy(src, dst, in_sem.at[3 + i])
        for i, (src, dst) in enumerate(
            ((live_hbm, live_all.at[z]), (rm_hbm, rm_ref), (cm_hbm, cm_ref))
        )
    ]
    for copy in small:
        copy.start()
    whole_u = pltpu.make_async_copy(u_hbm, u_ref, in_sem.at[1])
    whole_u.start()
    fronts = pltpu.make_async_copy(front_hbm, front_ref, in_sem.at[2])
    fronts.start()

    own_load = pltpu.make_async_copy(l_hbm, l_all.at[:, z], own_sem)
    pl.when(entry)(own_load.start)

    for copy in small:
        copy.wait()
    first.wait()
    pl.semaphore_wait(barrier, rows + 2)

    half = width // 2
    pieces = [slice(h * half, (h + 1) * half) for h in range(2)]

    def place(v, h):
        return remote(
            l_ref.at[v, pieces[h]], l_all.at[v, z, pieces[h]],
            l_send.at[v * (1 - h)], l_recv.at[v, h, z], {"row": c},
        )

    def cross(v, h):
        return remote(
            l_ref.at[v, pieces[h]], crossed.at[v, pieces[h]],
            l_send.at[v * (1 - h)], x_recv.at[v, h], {"col": far},
        )

    def onward(v, h):
        return remote(
            crossed.at[v, pieces[h]], l_all.at[v, z, pieces[h]],
            c_send, l_recv.at[v, h, z], {"row": far},
        )

    def routes(q):
        central = q * (last - q) > 0
        both = jnp.logical_and(jnp.logical_and(inner, central), q != z)
        one = jnp.logical_and(jnp.logical_and(at_end, central), (q - z) * (q - z) == 4)
        return both, jnp.logical_or(both, one)

    away = jnp.logical_not(entry)
    crosses, helps = routes(c), routes(far)
    places = [jnp.logical_and(away, jnp.logical_not(flag)) for flag in crosses]

    def launch(v):
        for h in range(2):
            pl.when(places[h])(lambda h=h: place(v, h).start())
            pl.when(crosses[h])(lambda h=h: cross(v, h).start())

    def carry_on(v):
        for h in range(2):
            @pl.when(helps[h])
            def _(h=h):
                cross(v, h).wait_recv()
                onward(v, h).start()

    live_out = []
    for step in range(1, rows):
        to = lax.rem(z + step, rows)
        live_out.append(remote(live_all.at[z], live_all.at[z], m_send, m_recv, {"row": to}))
        live_out[-1].start()
    rm_copy = remote(rm_ref, rm_in, rm_send, rm_recv, {"gz": other})
    rm_copy.start()
    gap = (z - c) * (z - c)
    to_end = c * (last - c) == 0
    distant = gap == 9
    late = jnp.logical_and(inner, jnp.logical_and(gap == 4, to_end))
    opener = jnp.logical_and(inner, jnp.logical_and(gap == 1, to_end))
    nearby = jnp.logical_and(away, jnp.logical_not(distant))
    lead = jnp.logical_and(nearby, jnp.logical_not(late))
    near_end, far_end = last * (1 - low), last * low
    next_in = low + (1 - low) * (last - 1)

    def deposit(v):
        return remote(l_ref.at[v], stash.at[v], l_send.at[0], f_recv.at[v], {"row": next_in})

    def pick_up(v, h):
        return remote(
            stash.at[v, pieces[h]], l_all.at[v, near_end, pieces[h]],
            g_send, l_recv.at[v, h, near_end], {"row": c},
        )

    @pl.when(distant)
    def _():
        for v in range(levels):
            deposit(v).start()

    @pl.when(lead)
    def _():
        for v in range(levels):
            launch(v)

    @pl.when(opener)
    def _():
        place(1, 0).wait_send()
        pl.semaphore_signal(turn, inc=1, device_id={"row": last - z}, device_id_type=MESH)

    @pl.when(late)
    def _():
        pl.semaphore_wait(turn, 1)
        launch(0)
        for v in range(levels):
            deposit(v).wait_recv()
            for h in range(2):
                pick_up(v, h).start()
        launch(1)

    def passes(v, a, h):
        spot = l_all.at[v, a, pieces[h]]
        post = remote(spot, spot, post_send.at[h], l_recv.at[v, h, a], {"col": far})
        relay = remote(spot, spot, relay_send, l_recv.at[v, h, a], {"col": mate})
        return post, relay

    count = rows - 1

    def place_of(k):
        mine = k // (levels * count)
        first = 1 - (k + levels) // (2 * levels)
        rest = k - levels
        v = first * k + (1 - first) * (rest // levels)
        step = lax.rem(rest + 2 * levels, levels)
        i = (1 - first) * (1 + step + v * (1 - 2 * step))
        near = (1 - depth) * (i + 1) + depth * (i + (i + 1) // 2)
        near = low * near + (1 - low) * (last - near)
        v = mine * (k - levels * count) + (1 - mine) * v
        return v, mine * z + (1 - mine) * near

    def turned(v, a, h):
        both = a == last - z
        return jnp.logical_and(inner, both if h == 0 else jnp.logical_or(both, (a - z) * (a - z) == 4))

    def spread(v, a, h):
        post, relay = passes(v, a, h)
        post.start()
        relay.start()

    def gather_entry(k):
        v, a = place_of(k)

        @pl.when(entry)
        def _():
            if k == levels * count:
                own_load.wait()
            for h in range(2):
                @pl.when(jnp.logical_not(turned(v, a, h)))
                def _(h=h):
                    pl.when(a != z)(lambda: passes(v, a, h)[1].wait_recv())
                    spread(v, a, h)

    def gather_second(k):
        v, a = place_of(k)
        for h in range(2):
            @pl.when(jnp.logical_and(second, turned(v, a, h)))
            def _(h=h):
                passes(v, a, h)[1].wait_recv()
                spread(v, a, h)

    def gather(k):
        gather_entry(k)
        gather_second(k)

    def take(k):
        v, a = place_of(k)

        def hand(h):
            relay = passes(v, a, h)[1]
            relay.wait_recv()
            relay.start()

        for h in range(2):
            there = turned(v, a, h)
            taken = jnp.logical_or(
                jnp.logical_and(second, jnp.logical_not(there)), jnp.logical_and(entry, there)
            )
            pl.when(taken)(lambda h=h: hand(h))

        @pl.when(jnp.logical_not(gate))
        def _():
            for h in range(2):
                passes(v, a, h)[1].wait_recv()

    def hop(v, a, l, side, row, to):
        slot = a + (rows - a) * side * (a == row).astype(jnp.int32)
        return remote(
            part.at[v, a, l], p_in.at[v, slot, l], p_send, p_recv.at[v, slot, l], {"row": to}
        )

    inward, outward = 1 - low, low
    across_mid = last - z

    def send(v, a, l):
        part[v, a, l] = own[v, a, l].astype(jnp.bfloat16)
        hop(v, a, l, inward, next_in, next_in).start()

    def item(k):
        v, a = place_of(k)
        block = l_all[v, a]
        to_layer = cm_ref[v]
        live = live_all[a, v]
        for j in range(CB):
            t = jnp.dot(
                block, u_ref[v, :, j * width : (j + 1) * width], preferred_element_type=jnp.float32
            )
            for l in range(layers):
                m = jnp.where(to_layer[:, j : j + 1] == l, live[:, j : j + 1], 0).astype(jnp.float32)
                if j == 0:
                    own[v, a, l] = t * m
                else:
                    own[v, a, l] += t * m


    gather_entry(0)
    carry_on(0)

    @pl.when(inner)
    def _():
        gather_entry(1)
        carry_on(1)
        gather(2)

    def flush(ref, sem):
        pltpu.make_async_copy(ref, ref, sem).wait()

    flush(live_all.at[: rows - 1], m_recv)
    whole_u.wait()
    rm_copy.wait()
    fronts.wait()

    def taken_in(v, a, l, side):
        slot = a + (rows - a) * side * (a == z).astype(jnp.int32)
        hop(v, a, l, side, z, z).wait_recv()
        return p_in[v, slot, l].astype(jnp.float32)

    def collect(v, l, side):
        own[v, z, l] += taken_in(v, z, l, side)

    def forward(v, a, l, side, to):
        part[v, a, l] = (own[v, a, l] + taken_in(v, a, l, side)).astype(jnp.bfloat16)
        hop(v, a, l, side, to, to).start()

    def way(v):
        return remote(y_out.at[v], y_in.at[v], y_send, y_recv.at[v], {"gz": other})

    def trade(v):
        y_out[v] = own[v, z, other].astype(jnp.bfloat16)
        way(v).start()

    def finish(v):
        mine = own[v, z, g].astype(jnp.bfloat16).astype(jnp.float32)
        way(v).wait_recv()
        theirs = y_in[v].astype(jnp.float32)
        for f in range(FRB):
            lines = slice(f * width, (f + 1) * width)
            here = (rm_ref[0, :, v : v + 1] == f).astype(jnp.float32)
            there = (rm_in[0, :, v : v + 1] == f).astype(jnp.float32)
            total = here * mine + there * theirs
            out_ref[v, lines, :] = (front_ref[v, lines, :].astype(jnp.float32) - total).astype(
                out_ref.dtype
            )


    def ahead(v, a, l):
        forward(v, a, l, inward, across_mid)

    def back(v, l):
        forward(v, near_end, l, outward, near_end)

    near, mid, end = next_in, last - next_in, last - z
    early = {
        0: ((0, near, other),),
        1: ((1, near, other),),
        2: ((0, mid, other),),
        3: ((0, end, other),),
        4: ((1, end, other), (0, end, g), (1, end, g)),
        5: ((1, mid, other), (0, mid, g), (1, mid, g), (0, near, g), (1, near, g)),
    }

    def edge_step(k):
        for v, a, l in early.get(k, ()):
            send(v, a, l)

    def edge_gather(k):
        if k < 5:
            gather_entry(k + 1)
        if k == 0:
            carry_on(1)
        if k == 5:
            gather_entry(6)
            gather_entry(7)

    def inner_gather(k):
        if k < 3:
            gather(k + 3)
        if k == 3:
            gather_entry(6)
            gather_entry(7)

    def shared_step(k):
        pl.when(at_end)(lambda: edge_gather(k))
        pl.when(inner)(lambda: inner_gather(k))

    def settle():
        some = p_in.at[0]
        flush(live_all.at[: rows - 1], m_send)
        pl.when(distant)(lambda: flush(some.at[:2], l_send.at[0]))
        pl.when(nearby)(lambda: flush(some.at[: rows - 1, 0], l_send.at[0]))
        single = jnp.logical_and(nearby, jnp.logical_not(opener))
        pl.when(single)(place(1, 0).wait_send)
        pl.when(late)(lambda: flush(some.at[:2], g_send))
        pl.when(helps[0])(lambda: flush(some.at[:2], c_send))
        only = jnp.logical_and(helps[1], jnp.logical_not(helps[0]))
        pl.when(only)(lambda: flush(some.at[0], c_send))

        @pl.when(gate)
        def _():
            flush(l_all, relay_send)

            @pl.when(jnp.logical_and(at_end, entry))
            def _():
                for h in range(2):
                    flush(some.at[:rows], post_send.at[h])

            @pl.when(jnp.logical_and(inner, entry))
            def _():
                flush(some.at[:3], post_send.at[0])
                flush(some.at[:2], post_send.at[1])

            @pl.when(jnp.logical_and(inner, second))
            def _():
                flush(some.at[0], post_send.at[0])
                flush(some.at[:2], post_send.at[1])

    def inner_step(k):
        if k == 3:
            ahead(0, across_mid, other)
            ahead(0, far_end, other)
        if k == 5:
            ahead(1, far_end, other)
            ahead(0, far_end, g)
            back(0, other)
        if k == 6:
            collect(0, other, inward)
            collect(0, other, outward)
            trade(0)
            ahead(1, far_end, g)
            back(1, other)
        if k == 7:
            ahead(1, across_mid, other)
            back(0, g)
            ahead(0, across_mid, g)
            back(1, g)
            collect(1, other, inward)
            collect(1, other, outward)
            trade(1)
            ahead(1, across_mid, g)
            settle()
            collect(0, g, outward)
            collect(0, g, inward)
            finish(0)
            collect(1, g, outward)
            collect(1, g, inward)

    def body(k, carry):
        take(k)
        item(k)
        for step in range(levels * rows):
            @pl.when(k == step)
            def _(step=step):
                pl.when(at_end)(lambda: edge_step(step))
                shared_step(step)
                pl.when(inner)(lambda: inner_step(step))

        return carry

    lax.fori_loop(0, levels * rows, body, 0)

    @pl.when(at_end)
    def _():
        collect(0, other, outward)
        trade(0)
        collect(1, other, outward)
        trade(1)
        collect(0, g, outward)
        settle()
        finish(0)
        collect(1, g, outward)

    finish(1)
    flush(p_in.at[:, : rows - 1], p_send)
    flush(y_out, y_send)


def stationary(rows, cols, layers, lpanel, upanel, rowmap, colmap, blockmask, front_blocks):
    levels, _, width, depth = lpanel.shape
    bf16 = jnp.bfloat16
    vmem = pl.BlockSpec(memory_space=pltpu.VMEM)
    hbm = pl.BlockSpec(memory_space=pl.ANY)
    dma = pltpu.SemaphoreType.DMA
    return pl.pallas_call(
        functools.partial(kernel, rows, cols, layers, levels, width),
        out_shape=pltpu.VMEM(front_blocks.shape, front_blocks.dtype),
        in_specs=[hbm] * 6,
        out_specs=vmem,
        scratch_shapes=[
            pltpu.VMEM(colmap.shape, jnp.int32),
            pltpu.VMEM((1, 1, levels), jnp.int32),
            pltpu.VMEM((levels, width, depth), bf16),
            pltpu.VMEM(upanel[:, 0].shape, bf16),
            pltpu.VMEM(front_blocks.shape, bf16),
            pltpu.VMEM((levels, width, depth), bf16),
            pltpu.VMEM((levels, width, depth), bf16),
            pltpu.VMEM((levels, rows, width, depth), bf16),
            pltpu.VMEM((rows,) + blockmask.shape[:1] + blockmask.shape[2:], jnp.int32),
            pltpu.VMEM((levels, rows, layers, width, width), jnp.float32),
            pltpu.VMEM((levels, rows, layers, width, width), bf16),
            pltpu.VMEM((levels, rows + 1, layers, width, width), bf16),
            pltpu.VMEM((levels, width, width), bf16),
            pltpu.VMEM((levels, width, width), bf16),
            pltpu.VMEM((1, 1, levels), jnp.int32),
            dma((6,)),
            dma,
            dma((levels, 2)),
            dma,
            dma((2,)),
            dma((levels, 2, rows)),
            dma((2,)),
            dma,
            dma,
            dma,
            dma,
            dma((levels, rows + 1, layers)),
            dma,
            dma((levels,)),
            dma,
            dma,
            pltpu.SemaphoreType.REGULAR,
            dma((levels,)),
            dma,
        ],
        compiler_params=pltpu.CompilerParams(collective_id=0, has_side_effects=True),
    )(
        lpanel[:, 0], upanel[:, 0], colmap, blockmask[:, 0], jnp.transpose(rowmap, (1, 2, 0)),
        front_blocks,
    )


def solution(mesh):
    rows, cols, layers = mesh.shape["row"], mesh.shape["col"], mesh.shape["gz"]
    body = general
    if rows == cols == 2 * layers and layers == 2:
        body = functools.partial(stationary, rows, cols, layers)
    return jax.shard_map(
        body,
        mesh=mesh,
        in_specs=(
            P(None, "gz", "row", "col"),
            P(None, "gz", "row", "col"),
            P(None, "gz", "row"),
            P(None, "gz", "col"),
            P(None, "gz", "row", "col"),
            P(None, "row", ("gz", "col")),
        ),
        out_specs=P(None, "row", ("gz", "col")),
        check_vma=False,
    )
```

```python
import functools

import jax
import jax.numpy as jnp
from jax import lax
from jax.experimental import pallas as pl
from jax.experimental.pallas import tpu as pltpu
from jax.sharding import PartitionSpec as P

CB = 4
FRB = 2
MESH = pl.DeviceIdType.MESH


def column_sums(schur, cols_of, live, layers):
    width = schur.shape[0]
    blocks = schur.reshape(width, CB, width)
    targets = cols_of[:, None] == jnp.arange(layers, dtype=jnp.int32)[None, :]
    col_select = targets.astype(jnp.float32) * live.astype(jnp.float32)[:, None]
    return jnp.einsum("bjk,jl->lbk", blocks, col_select, precision=lax.Precision.HIGHEST)


def general(lpanel, upanel, rowmap, colmap, blockmask, front_blocks):
    layers = lax.axis_size("gz")
    width = lpanel.shape[2]
    levels = lpanel.shape[0]
    tiles = []
    for depth in range(levels):
        left_rows = lax.all_gather(lpanel[depth, 0], "col", axis=1, tiled=True)
        tiles.append(
            jnp.dot(
                left_rows,
                lax.all_gather(upanel[depth, 0], "row", axis=0, tiled=True),
                preferred_element_type=jnp.float32,
            )
        )
    results = []
    every_row = lax.all_gather(rowmap[:, :, 0], "gz", axis=1, tiled=True)
    for depth in range(levels):
        sums = column_sums(tiles[depth], colmap[depth, 0], blockmask[depth, 0, 0], layers).astype(
            jnp.bfloat16
        )
        arrived = lax.all_to_all(sums, "gz", split_axis=0, concat_axis=0, tiled=True)
        row_select = (
            every_row[depth][:, None] == jnp.arange(FRB, dtype=jnp.int32)[None, :]
        ).astype(jnp.float32)
        placed = jnp.einsum(
            "sf,sbk->fbk", row_select, arrived.astype(jnp.float32), precision=lax.Precision.HIGHEST
        )
        placed = placed.reshape(FRB * width, width)
        results.append((front_blocks[depth].astype(jnp.float32) - placed).astype(jnp.bfloat16))
    return jnp.stack(results)


def kernel(
    rows, cols, layers, levels, width,
    l_hbm, u_hbm, cm_hbm, live_hbm, rm_hbm, front_hbm, out_ref,
    cm_ref, rm_ref,
    l_ref, u_ref, front_ref, crossed, stash, l_all, live_all, own, part, p_in, y_out, y_in, rm_in,
    in_sem, own_sem, x_recv, c_send, l_send, l_recv, post_send, relay_send,
    m_send, m_recv, p_send, p_recv, y_send, y_recv, rm_send, rm_recv, turn, f_recv, g_send,
):
    z = lax.axis_index("row")
    c = lax.axis_index("col")
    g = lax.axis_index("gz")
    far = lax.rem(c + cols // 2, cols)
    mate = c + 1 - 2 * lax.rem(c, 2)
    other = 1 - g
    last = rows - 1
    entry, second = c == z, far == z
    gate = jnp.logical_or(entry, second)
    low = 1 - z // (rows // 2)
    depth = low * z + (1 - low) * (last - z)
    at_end = depth == 0
    inner = jnp.logical_not(at_end)

    def remote(src, dst, send, recv, where):
        return pltpu.make_async_remote_copy(
            src_ref=src, dst_ref=dst, send_sem=send, recv_sem=recv,
            device_id=where, device_id_type=MESH,
        )

    barrier = pltpu.get_barrier_semaphore()
    for step in range(1, rows):
        pl.semaphore_signal(
            barrier, inc=1, device_id={"row": lax.rem(z + step, rows)}, device_id_type=MESH
        )
    pl.semaphore_signal(barrier, inc=1, device_id={"col": far}, device_id_type=MESH)
    pl.semaphore_signal(barrier, inc=1, device_id={"col": mate}, device_id_type=MESH)
    pl.semaphore_signal(barrier, inc=1, device_id={"gz": other}, device_id_type=MESH)

    first = pltpu.make_async_copy(l_hbm, l_ref, in_sem.at[0])
    first.start()
    small = [
        pltpu.make_async_copy(src, dst, in_sem.at[3 + i])
        for i, (src, dst) in enumerate(
            ((live_hbm, live_all.at[z]), (rm_hbm, rm_ref), (cm_hbm, cm_ref))
        )
    ]
    for copy in small:
        copy.start()
    whole_u = pltpu.make_async_copy(u_hbm, u_ref, in_sem.at[1])
    whole_u.start()
    fronts = pltpu.make_async_copy(front_hbm, front_ref, in_sem.at[2])
    fronts.start()

    own_load = pltpu.make_async_copy(l_hbm, l_all.at[:, z], own_sem)
    pl.when(entry)(own_load.start)

    for copy in small:
        copy.wait()
    first.wait()
    pl.semaphore_wait(barrier, rows + 2)

    parts = 4
    lines = width // parts
    pieces = [slice(h * lines, (h + 1) * lines) for h in range(parts)]
    halves = [slice(h * 2 * lines, (h + 1) * 2 * lines) for h in range(2)]

    def place(v, h):
        return remote(
            l_ref.at[v, pieces[h]], l_all.at[v, z, pieces[h]],
            l_send.at[int(v == 1 and h == 0)], l_recv.at[v, h, z], {"row": c},
        )

    def cross(v, h):
        return remote(
            l_ref.at[v, halves[h]], crossed.at[v, halves[h]],
            l_send.at[v * (1 - h)], x_recv.at[v, h], {"col": far},
        )

    def onward(v, h):
        return remote(
            crossed.at[v, pieces[h]], l_all.at[v, z, pieces[h]],
            c_send, l_recv.at[v, h, z], {"row": far},
        )

    def routes(q):
        central = q * (last - q) > 0
        both = jnp.logical_and(jnp.logical_and(inner, central), q != z)
        one = jnp.logical_and(jnp.logical_and(at_end, central), (q - z) * (q - z) == 4)
        return both, jnp.logical_or(both, one)

    away = jnp.logical_not(entry)
    crosses, helps = routes(c), routes(far)
    places = [jnp.logical_and(away, jnp.logical_not(flag)) for flag in crosses]

    def launch(v):
        for h in range(2):
            pl.when(crosses[h])(lambda h=h: cross(v, h).start())
        for h in range(parts):
            pl.when(places[h // 2])(lambda h=h: place(v, h).start())

    def carry_on(v):
        for h in range(2):
            @pl.when(helps[h])
            def _(h=h):
                cross(v, h).wait_recv()
                for n in range(2):
                    onward(v, 2 * h + n).start()

    live_out = []
    for step in range(1, rows):
        to = lax.rem(z + step, rows)
        live_out.append(remote(live_all.at[z], live_all.at[z], m_send, m_recv, {"row": to}))
        live_out[-1].start()
    rm_copy = remote(rm_ref, rm_in, rm_send, rm_recv, {"gz": other})
    rm_copy.start()
    gap = (z - c) * (z - c)
    to_end = c * (last - c) == 0
    distant = gap == 9
    late = jnp.logical_and(inner, jnp.logical_and(gap == 4, to_end))
    opener = jnp.logical_and(inner, jnp.logical_and(gap == 1, to_end))
    nearby = jnp.logical_and(away, jnp.logical_not(distant))
    lead = jnp.logical_and(nearby, jnp.logical_not(late))
    near_end, far_end = last * (1 - low), last * low
    next_in = low + (1 - low) * (last - 1)

    def deposit(v):
        return remote(l_ref.at[v], stash.at[v], l_send.at[0], f_recv.at[v], {"row": next_in})

    def pick_up(v, h):
        return remote(
            stash.at[v, pieces[h]], l_all.at[v, near_end, pieces[h]],
            g_send, l_recv.at[v, h, near_end], {"row": c},
        )

    @pl.when(distant)
    def _():
        for v in range(levels):
            deposit(v).start()

    @pl.when(lead)
    def _():
        for v in range(levels):
            launch(v)

    @pl.when(opener)
    def _():
        place(1, 0).wait_send()
        pl.semaphore_signal(turn, inc=1, device_id={"row": last - z}, device_id_type=MESH)

    @pl.when(late)
    def _():
        pl.semaphore_wait(turn, 1)
        launch(0)
        for v in range(levels):
            deposit(v).wait_recv()
            for h in range(parts):
                pick_up(v, h).start()
        launch(1)

    def passes(v, a, h):
        spot = l_all.at[v, a, pieces[h]]
        post = remote(spot, spot, post_send.at[h // 2], l_recv.at[v, h, a], {"col": far})
        relay = remote(spot, spot, relay_send, l_recv.at[v, h, a], {"col": mate})
        return post, relay

    count = rows - 1

    def place_of(k):
        mine = k // (levels * count)
        first = 1 - (k + levels) // (2 * levels)
        rest = k - levels
        v = first * k + (1 - first) * (rest // levels)
        step = lax.rem(rest + 2 * levels, levels)
        i = (1 - first) * (1 + step + v * (1 - 2 * step))
        near = (1 - depth) * (i + 1) + depth * (i + (i + 1) // 2)
        near = low * near + (1 - low) * (last - near)
        v = mine * (k - levels * count) + (1 - mine) * v
        return v, mine * z + (1 - mine) * near

    def turned(v, a, h):
        both = a == last - z
        return jnp.logical_and(inner, both if h < 2 else jnp.logical_or(both, (a - z) * (a - z) == 4))

    def spread(v, a, h):
        post, relay = passes(v, a, h)
        post.start()
        relay.start()

    def gather_entry(k):
        v, a = place_of(k)

        @pl.when(entry)
        def _():
            if k == levels * count:
                own_load.wait()
            for h in range(parts):
                @pl.when(jnp.logical_not(turned(v, a, h)))
                def _(h=h):
                    pl.when(a != z)(lambda: passes(v, a, h)[1].wait_recv())
                    spread(v, a, h)

    def gather_second(k):
        v, a = place_of(k)
        for h in range(parts):
            @pl.when(jnp.logical_and(second, turned(v, a, h)))
            def _(h=h):
                passes(v, a, h)[1].wait_recv()
                spread(v, a, h)

    def gather(k):
        gather_entry(k)
        gather_second(k)

    def take(k):
        v, a = place_of(k)

        def hand(h):
            relay = passes(v, a, h)[1]
            relay.wait_recv()
            relay.start()

        for h in range(parts):
            there = turned(v, a, h)
            taken = jnp.logical_or(
                jnp.logical_and(second, jnp.logical_not(there)), jnp.logical_and(entry, there)
            )
            pl.when(taken)(lambda h=h: hand(h))

        @pl.when(jnp.logical_not(gate))
        def _():
            for h in range(parts):
                passes(v, a, h)[1].wait_recv()

    def hop(v, a, l, side, row, to):
        slot = a + (rows - a) * side * (a == row).astype(jnp.int32)
        return remote(
            part.at[v, a, l], p_in.at[v, slot, l], p_send, p_recv.at[v, slot, l], {"row": to}
        )

    inward, outward = 1 - low, low
    across_mid = last - z

    def send(v, a, l):
        part[v, a, l] = own[v, a, l].astype(jnp.bfloat16)
        hop(v, a, l, inward, next_in, next_in).start()

    def item(k):
        v, a = place_of(k)
        block = l_all[v, a]
        to_layer = cm_ref[v]
        live = live_all[a, v]
        for j in range(CB):
            t = jnp.dot(
                block, u_ref[v, :, j * width : (j + 1) * width], preferred_element_type=jnp.float32
            )
            for l in range(layers):
                m = jnp.where(to_layer[:, j : j + 1] == l, live[:, j : j + 1], 0).astype(jnp.float32)
                if j == 0:
                    own[v, a, l] = t * m
                else:
                    own[v, a, l] += t * m


    gather_entry(0)
    carry_on(0)

    @pl.when(inner)
    def _():
        gather_entry(1)
        carry_on(1)
        gather(2)

    def flush(ref, sem):
        pltpu.make_async_copy(ref, ref, sem).wait()

    flush(live_all.at[: rows - 1], m_recv)
    whole_u.wait()
    rm_copy.wait()
    fronts.wait()

    def taken_in(v, a, l, side):
        slot = a + (rows - a) * side * (a == z).astype(jnp.int32)
        hop(v, a, l, side, z, z).wait_recv()
        return p_in[v, slot, l].astype(jnp.float32)

    def collect(v, l, side):
        own[v, z, l] += taken_in(v, z, l, side)

    def forward(v, a, l, side, to):
        part[v, a, l] = (own[v, a, l] + taken_in(v, a, l, side)).astype(jnp.bfloat16)
        hop(v, a, l, side, to, to).start()

    def way(v):
        return remote(y_out.at[v], y_in.at[v], y_send, y_recv.at[v], {"gz": other})

    def trade(v):
        y_out[v] = own[v, z, other].astype(jnp.bfloat16)
        way(v).start()

    def finish(v):
        mine = own[v, z, g].astype(jnp.bfloat16).astype(jnp.float32)
        way(v).wait_recv()
        theirs = y_in[v].astype(jnp.float32)
        for f in range(FRB):
            lines = slice(f * width, (f + 1) * width)
            here = (rm_ref[0, :, v : v + 1] == f).astype(jnp.float32)
            there = (rm_in[0, :, v : v + 1] == f).astype(jnp.float32)
            total = here * mine + there * theirs
            out_ref[v, lines, :] = (front_ref[v, lines, :].astype(jnp.float32) - total).astype(
                out_ref.dtype
            )


    def ahead(v, a, l):
        forward(v, a, l, inward, across_mid)

    def back(v, l):
        forward(v, near_end, l, outward, near_end)

    near, mid, end = next_in, last - next_in, last - z
    early = {
        0: ((0, near, other),),
        1: ((1, near, other),),
        2: ((0, mid, other),),
        3: ((0, end, other),),
        4: ((1, end, other), (0, end, g), (1, end, g)),
        5: ((1, mid, other), (0, mid, g), (1, mid, g), (0, near, g), (1, near, g)),
    }

    def edge_step(k):
        for v, a, l in early.get(k, ()):
            send(v, a, l)

    def edge_gather(k):
        if k < 5:
            gather_entry(k + 1)
        if k == 0:
            carry_on(1)
        if k == 5:
            gather_entry(6)
            gather_entry(7)

    def inner_gather(k):
        if k < 3:
            gather(k + 3)
        if k == 3:
            gather_entry(6)
            gather_entry(7)

    def shared_step(k):
        pl.when(at_end)(lambda: edge_gather(k))
        pl.when(inner)(lambda: inner_gather(k))

    def settle():
        some = p_in.at[0]
        flush(live_all.at[: rows - 1], m_send)
        pl.when(distant)(lambda: flush(some.at[:2], l_send.at[0]))
        count_a = jnp.logical_and(nearby, jnp.logical_not(crosses[0]))
        count_b = jnp.logical_and(nearby, crosses[0])
        pl.when(count_a)(lambda: flush(u_ref.at[0, : 7 * lines // 2], l_send.at[0]))
        pl.when(count_b)(lambda: flush(some.at[: rows - 1, 0], l_send.at[0]))
        pl.when(count_b)(lambda: flush(some.at[0, 0], l_send.at[1]))
        single = jnp.logical_and(count_a, jnp.logical_not(opener))
        pl.when(single)(place(1, 0).wait_send)
        pl.when(late)(lambda: flush(some.at[:2], g_send))
        pl.when(helps[0])(lambda: flush(some.at[:2], c_send))
        only = jnp.logical_and(helps[1], jnp.logical_not(helps[0]))
        pl.when(only)(lambda: flush(some.at[0], c_send))

        @pl.when(gate)
        def _():
            flush(l_all, relay_send)

            @pl.when(jnp.logical_and(at_end, entry))
            def _():
                for h in range(2):
                    flush(some.at[:rows], post_send.at[h])

            @pl.when(jnp.logical_and(inner, entry))
            def _():
                flush(some.at[:3], post_send.at[0])
                flush(some.at[:2], post_send.at[1])

            @pl.when(jnp.logical_and(inner, second))
            def _():
                flush(some.at[0], post_send.at[0])
                flush(some.at[:2], post_send.at[1])

    def inner_step(k):
        if k == 3:
            ahead(0, across_mid, other)
            ahead(0, far_end, other)
        if k == 5:
            ahead(1, far_end, other)
            ahead(0, far_end, g)
            back(0, other)
        if k == 6:
            collect(0, other, inward)
            collect(0, other, outward)
            trade(0)
            ahead(1, far_end, g)
            back(1, other)
        if k == 7:
            ahead(1, across_mid, other)
            back(0, g)
            ahead(0, across_mid, g)
            back(1, g)
            collect(1, other, inward)
            collect(1, other, outward)
            trade(1)
            ahead(1, across_mid, g)
            settle()
            collect(0, g, outward)
            collect(0, g, inward)
            finish(0)
            collect(1, g, outward)
            collect(1, g, inward)

    def body(k, carry):
        take(k)
        item(k)
        for step in range(levels * rows):
            @pl.when(k == step)
            def _(step=step):
                pl.when(at_end)(lambda: edge_step(step))
                shared_step(step)
                pl.when(inner)(lambda: inner_step(step))

        return carry

    lax.fori_loop(0, levels * rows, body, 0)

    @pl.when(at_end)
    def _():
        collect(0, other, outward)
        trade(0)
        collect(1, other, outward)
        trade(1)
        collect(0, g, outward)
        settle()
        finish(0)
        collect(1, g, outward)

    finish(1)
    flush(p_in.at[:, : rows - 1], p_send)
    flush(y_out, y_send)


def stationary(rows, cols, layers, lpanel, upanel, rowmap, colmap, blockmask, front_blocks):
    levels, _, width, depth = lpanel.shape
    bf16 = jnp.bfloat16
    vmem = pl.BlockSpec(memory_space=pltpu.VMEM)
    hbm = pl.BlockSpec(memory_space=pl.ANY)
    dma = pltpu.SemaphoreType.DMA
    return pl.pallas_call(
        functools.partial(kernel, rows, cols, layers, levels, width),
        out_shape=pltpu.VMEM(front_blocks.shape, front_blocks.dtype),
        in_specs=[hbm] * 6,
        out_specs=vmem,
        scratch_shapes=[
            pltpu.VMEM(colmap.shape, jnp.int32),
            pltpu.VMEM((1, 1, levels), jnp.int32),
            pltpu.VMEM((levels, width, depth), bf16),
            pltpu.VMEM(upanel[:, 0].shape, bf16),
            pltpu.VMEM(front_blocks.shape, bf16),
            pltpu.VMEM((levels, width, depth), bf16),
            pltpu.VMEM((levels, width, depth), bf16),
            pltpu.VMEM((levels, rows, width, depth), bf16),
            pltpu.VMEM((rows,) + blockmask.shape[:1] + blockmask.shape[2:], jnp.int32),
            pltpu.VMEM((levels, rows, layers, width, width), jnp.float32),
            pltpu.VMEM((levels, rows, layers, width, width), bf16),
            pltpu.VMEM((levels, rows + 1, layers, width, width), bf16),
            pltpu.VMEM((levels, width, width), bf16),
            pltpu.VMEM((levels, width, width), bf16),
            pltpu.VMEM((1, 1, levels), jnp.int32),
            dma((6,)),
            dma,
            dma((levels, 2)),
            dma,
            dma((2,)),
            dma((levels, 4, rows)),
            dma((2,)),
            dma,
            dma,
            dma,
            dma,
            dma((levels, rows + 1, layers)),
            dma,
            dma((levels,)),
            dma,
            dma,
            pltpu.SemaphoreType.REGULAR,
            dma((levels,)),
            dma,
        ],
        compiler_params=pltpu.CompilerParams(collective_id=0, has_side_effects=True),
    )(
        lpanel[:, 0], upanel[:, 0], colmap, blockmask[:, 0], jnp.transpose(rowmap, (1, 2, 0)),
        front_blocks,
    )


def solution(mesh):
    rows, cols, layers = mesh.shape["row"], mesh.shape["col"], mesh.shape["gz"]
    body = general
    if rows == cols == 2 * layers and layers == 2:
        body = functools.partial(stationary, rows, cols, layers)
    return jax.shard_map(
        body,
        mesh=mesh,
        in_specs=(
            P(None, "gz", "row", "col"),
            P(None, "gz", "row", "col"),
            P(None, "gz", "row"),
            P(None, "gz", "col"),
            P(None, "gz", "row", "col"),
            P(None, "row", ("gz", "col")),
        ),
        out_specs=P(None, "row", ("gz", "col")),
        check_vma=False,
    )
```

```python
import functools

import jax
import jax.numpy as jnp
from jax import lax
from jax.experimental import pallas as pl
from jax.experimental.pallas import tpu as pltpu
from jax.sharding import PartitionSpec as P

CB = 4
FRB = 2
MESH = pl.DeviceIdType.MESH


def column_sums(schur, cols_of, live, layers):
    width = schur.shape[0]
    blocks = schur.reshape(width, CB, width)
    targets = cols_of[:, None] == jnp.arange(layers, dtype=jnp.int32)[None, :]
    col_select = targets.astype(jnp.float32) * live.astype(jnp.float32)[:, None]
    return jnp.einsum("bjk,jl->lbk", blocks, col_select, precision=lax.Precision.HIGHEST)


def general(lpanel, upanel, rowmap, colmap, blockmask, front_blocks):
    layers = lax.axis_size("gz")
    width = lpanel.shape[2]
    levels = lpanel.shape[0]
    tiles = []
    for depth in range(levels):
        left_rows = lax.all_gather(lpanel[depth, 0], "col", axis=1, tiled=True)
        tiles.append(
            jnp.dot(
                left_rows,
                lax.all_gather(upanel[depth, 0], "row", axis=0, tiled=True),
                preferred_element_type=jnp.float32,
            )
        )
    results = []
    every_row = lax.all_gather(rowmap[:, :, 0], "gz", axis=1, tiled=True)
    for depth in range(levels):
        sums = column_sums(tiles[depth], colmap[depth, 0], blockmask[depth, 0, 0], layers).astype(
            jnp.bfloat16
        )
        arrived = lax.all_to_all(sums, "gz", split_axis=0, concat_axis=0, tiled=True)
        row_select = (
            every_row[depth][:, None] == jnp.arange(FRB, dtype=jnp.int32)[None, :]
        ).astype(jnp.float32)
        placed = jnp.einsum(
            "sf,sbk->fbk", row_select, arrived.astype(jnp.float32), precision=lax.Precision.HIGHEST
        )
        placed = placed.reshape(FRB * width, width)
        results.append((front_blocks[depth].astype(jnp.float32) - placed).astype(jnp.bfloat16))
    return jnp.stack(results)


def kernel(
    rows, cols, layers, levels, width,
    l_hbm, u_hbm, cm_hbm, live_hbm, rm_hbm, front_hbm, out_ref,
    cm_ref, rm_ref,
    l_ref, u_ref, front_ref, crossed, stash, l_all, live_all, own, part, p_in, y_out, y_in, rm_in,
    in_sem, own_sem, x_recv, c_send, l_send, l_recv, post_send, relay_send,
    m_send, m_recv, p_send, p_recv, y_send, y_recv, rm_send, rm_recv, turn, f_recv, g_send,
):
    z = lax.axis_index("row")
    c = lax.axis_index("col")
    g = lax.axis_index("gz")
    far = lax.rem(c + cols // 2, cols)
    mate = c + 1 - 2 * lax.rem(c, 2)
    other = 1 - g
    last = rows - 1
    entry, second = c == z, far == z
    gate = jnp.logical_or(entry, second)
    low = 1 - z // (rows // 2)
    depth = low * z + (1 - low) * (last - z)
    at_end = depth == 0
    inner = jnp.logical_not(at_end)

    def remote(src, dst, send, recv, where):
        return pltpu.make_async_remote_copy(
            src_ref=src, dst_ref=dst, send_sem=send, recv_sem=recv,
            device_id=where, device_id_type=MESH,
        )

    barrier = pltpu.get_barrier_semaphore()
    for step in range(1, rows):
        pl.semaphore_signal(
            barrier, inc=1, device_id={"row": lax.rem(z + step, rows)}, device_id_type=MESH
        )
    pl.semaphore_signal(barrier, inc=1, device_id={"col": far}, device_id_type=MESH)
    pl.semaphore_signal(barrier, inc=1, device_id={"col": mate}, device_id_type=MESH)
    pl.semaphore_signal(barrier, inc=1, device_id={"gz": other}, device_id_type=MESH)

    first = pltpu.make_async_copy(l_hbm, l_ref, in_sem.at[0])
    first.start()
    small = [
        pltpu.make_async_copy(src, dst, in_sem.at[3 + i])
        for i, (src, dst) in enumerate(
            ((live_hbm, live_all.at[z]), (rm_hbm, rm_ref), (cm_hbm, cm_ref))
        )
    ]
    for copy in small:
        copy.start()
    whole_u = pltpu.make_async_copy(u_hbm, u_ref, in_sem.at[1])
    whole_u.start()
    fronts = pltpu.make_async_copy(front_hbm, front_ref, in_sem.at[2])
    fronts.start()

    own_load = pltpu.make_async_copy(l_hbm, l_all.at[:, z], own_sem)
    pl.when(entry)(own_load.start)

    for copy in small:
        copy.wait()
    first.wait()
    pl.semaphore_wait(barrier, rows + 2)

    parts = 4
    lines = width // parts
    pieces = [slice(h * lines, (h + 1) * lines) for h in range(parts)]
    halves = [slice(h * 2 * lines, (h + 1) * 2 * lines) for h in range(2)]

    def place(v, h):
        return remote(
            l_ref.at[v, pieces[h]], l_all.at[v, z, pieces[h]],
            l_send.at[int(v == 1 and h == 0)], l_recv.at[v, h, z], {"row": c},
        )

    def cross(v, h):
        return remote(
            l_ref.at[v, halves[h]], crossed.at[v, halves[h]],
            l_send.at[v * (1 - h)], x_recv.at[v, h], {"col": far},
        )

    def onward(v, h):
        return remote(
            crossed.at[v, pieces[h]], l_all.at[v, z, pieces[h]],
            c_send, l_recv.at[v, h, z], {"row": far},
        )

    def routes(q):
        central = q * (last - q) > 0
        both = jnp.logical_and(jnp.logical_and(inner, central), q != z)
        one = jnp.logical_and(jnp.logical_and(at_end, central), (q - z) * (q - z) == 4)
        return both, jnp.logical_or(both, one)

    away = jnp.logical_not(entry)
    crosses, helps = routes(c), routes(far)
    places = [jnp.logical_and(away, jnp.logical_not(flag)) for flag in crosses]

    def launch(v):
        for h in range(2):
            pl.when(crosses[h])(lambda h=h: cross(v, h).start())
        for h in range(parts):
            pl.when(places[h // 2])(lambda h=h: place(v, h).start())

    def carry_on(v):
        for h in range(2):
            @pl.when(helps[h])
            def _(h=h):
                cross(v, h).wait_recv()
                for n in range(2):
                    onward(v, 2 * h + n).start()

    live_out = []
    for step in range(1, rows):
        to = lax.rem(z + step, rows)
        live_out.append(remote(live_all.at[z], live_all.at[z], m_send, m_recv, {"row": to}))
        live_out[-1].start()
    rm_copy = remote(rm_ref, rm_in, rm_send, rm_recv, {"gz": other})
    rm_copy.start()
    gap = (z - c) * (z - c)
    to_end = c * (last - c) == 0
    distant = gap == 9
    late = jnp.logical_and(inner, jnp.logical_and(gap == 4, to_end))
    opener = jnp.logical_and(inner, jnp.logical_and(gap == 1, to_end))
    nearby = jnp.logical_and(away, jnp.logical_not(distant))
    lead = jnp.logical_and(nearby, jnp.logical_not(late))
    near_end, far_end = last * (1 - low), last * low
    next_in = low + (1 - low) * (last - 1)

    def deposit(v):
        return remote(l_ref.at[v], stash.at[v], l_send.at[0], f_recv.at[v], {"row": next_in})

    def pick_up(v, h):
        return remote(
            stash.at[v, pieces[h]], l_all.at[v, near_end, pieces[h]],
            g_send, l_recv.at[v, h, near_end], {"row": c},
        )

    @pl.when(distant)
    def _():
        for v in range(levels):
            deposit(v).start()

    @pl.when(lead)
    def _():
        for v in range(levels):
            launch(v)

    @pl.when(opener)
    def _():
        place(1, 0).wait_send()
        pl.semaphore_signal(turn, inc=1, device_id={"row": last - z}, device_id_type=MESH)

    @pl.when(late)
    def _():
        pl.semaphore_wait(turn, 1)
        launch(0)
        for v in range(levels):
            deposit(v).wait_recv()
            for h in range(parts):
                pick_up(v, h).start()
        launch(1)

    def passes(v, a, h):
        spot = l_all.at[v, a, pieces[h]]
        post = remote(spot, spot, post_send.at[h // 2], l_recv.at[v, h, a], {"col": far})
        relay = remote(spot, spot, relay_send, l_recv.at[v, h, a], {"col": mate})
        return post, relay

    count = rows - 1

    def place_of(k):
        mine = k // (levels * count)
        first = 1 - (k + levels) // (2 * levels)
        rest = k - levels
        v = first * k + (1 - first) * (rest // levels)
        step = lax.rem(rest + 2 * levels, levels)
        i = (1 - first) * (1 + step + v * (1 - 2 * step))
        near = (1 - depth) * (i + 1) + depth * (i + (i + 1) // 2)
        near = low * near + (1 - low) * (last - near)
        v = mine * (k - levels * count) + (1 - mine) * v
        return v, mine * z + (1 - mine) * near

    def turned(v, a, h):
        both = a == last - z
        return jnp.logical_and(inner, both if h < 2 else jnp.logical_or(both, (a - z) * (a - z) == 4))

    def spread(v, a, h):
        post, relay = passes(v, a, h)
        post.start()
        relay.start()

    def gather_entry(k):
        v, a = place_of(k)

        @pl.when(entry)
        def _():
            if k == levels * count:
                own_load.wait()
            for h in range(parts):
                @pl.when(jnp.logical_not(turned(v, a, h)))
                def _(h=h):
                    pl.when(a != z)(lambda: passes(v, a, h)[1].wait_recv())
                    spread(v, a, h)

    def gather_second(k):
        v, a = place_of(k)
        for h in range(parts):
            @pl.when(jnp.logical_and(second, turned(v, a, h)))
            def _(h=h):
                passes(v, a, h)[1].wait_recv()
                spread(v, a, h)

    def gather(k):
        gather_entry(k)
        gather_second(k)

    def take(k, part_of):
        v, a = place_of(k)

        def hand(h):
            relay = passes(v, a, h)[1]
            relay.wait_recv()
            relay.start()

        for h in part_of:
            there = turned(v, a, h)
            taken = jnp.logical_or(
                jnp.logical_and(second, jnp.logical_not(there)), jnp.logical_and(entry, there)
            )
            pl.when(taken)(lambda h=h: hand(h))

        @pl.when(jnp.logical_not(gate))
        def _():
            for h in part_of:
                passes(v, a, h)[1].wait_recv()

    def hop(v, a, l, side, row, to):
        slot = a + (rows - a) * side * (a == row).astype(jnp.int32)
        return remote(
            part.at[v, a, l], p_in.at[v, slot, l], p_send, p_recv.at[v, slot, l], {"row": to}
        )

    inward, outward = 1 - low, low
    across_mid = last - z

    def send(v, a, l):
        part[v, a, l] = own[v, a, l].astype(jnp.bfloat16)
        hop(v, a, l, inward, next_in, next_in).start()

    def item(k, lane):
        v, a = place_of(k)
        block = l_all[v, a, lane, :]
        to_layer = cm_ref[v]
        live = live_all[a, v]
        for j in range(CB):
            t = jnp.dot(
                block, u_ref[v, :, j * width : (j + 1) * width], preferred_element_type=jnp.float32
            )
            for l in range(layers):
                m = jnp.where(to_layer[:, j : j + 1] == l, live[:, j : j + 1], 0).astype(jnp.float32)
                if j == 0:
                    own[v, a, l, lane, :] = t * m
                else:
                    own[v, a, l, lane, :] += t * m

    gather_entry(0)
    carry_on(0)

    @pl.when(inner)
    def _():
        gather_entry(1)
        carry_on(1)
        gather(2)

    def flush(ref, sem):
        pltpu.make_async_copy(ref, ref, sem).wait()

    flush(live_all.at[: rows - 1], m_recv)
    whole_u.wait()
    rm_copy.wait()
    fronts.wait()

    def taken_in(v, a, l, side):
        slot = a + (rows - a) * side * (a == z).astype(jnp.int32)
        hop(v, a, l, side, z, z).wait_recv()
        return p_in[v, slot, l].astype(jnp.float32)

    def collect(v, l, side):
        own[v, z, l] += taken_in(v, z, l, side)

    def forward(v, a, l, side, to):
        part[v, a, l] = (own[v, a, l] + taken_in(v, a, l, side)).astype(jnp.bfloat16)
        hop(v, a, l, side, to, to).start()

    def way(v):
        return remote(y_out.at[v], y_in.at[v], y_send, y_recv.at[v], {"gz": other})

    def trade(v):
        y_out[v] = own[v, z, other].astype(jnp.bfloat16)
        way(v).start()

    def finish(v):
        mine = own[v, z, g].astype(jnp.bfloat16).astype(jnp.float32)
        way(v).wait_recv()
        theirs = y_in[v].astype(jnp.float32)
        for f in range(FRB):
            lines = slice(f * width, (f + 1) * width)
            here = (rm_ref[0, :, v : v + 1] == f).astype(jnp.float32)
            there = (rm_in[0, :, v : v + 1] == f).astype(jnp.float32)
            total = here * mine + there * theirs
            out_ref[v, lines, :] = (front_ref[v, lines, :].astype(jnp.float32) - total).astype(
                out_ref.dtype
            )


    def ahead(v, a, l):
        forward(v, a, l, inward, across_mid)

    def back(v, l):
        forward(v, near_end, l, outward, near_end)

    near, mid, end = next_in, last - next_in, last - z
    early = {
        0: ((0, near, other),),
        1: ((1, near, other),),
        2: ((0, mid, other),),
        3: ((0, end, other),),
        4: ((1, end, other), (0, end, g), (1, end, g)),
        5: ((1, mid, other), (0, mid, g), (1, mid, g), (0, near, g), (1, near, g)),
    }

    def edge_step(k):
        for v, a, l in early.get(k, ()):
            send(v, a, l)

    def edge_gather(k):
        if k < 5:
            gather_entry(k + 1)
        if k == 0:
            carry_on(1)
        if k == 5:
            gather_entry(6)
            gather_entry(7)

    def inner_gather(k):
        if k < 3:
            gather(k + 3)
        if k == 3:
            gather_entry(6)
            gather_entry(7)

    def shared_step(k):
        pl.when(at_end)(lambda: edge_gather(k))
        pl.when(inner)(lambda: inner_gather(k))

    def settle():
        some = p_in.at[0]
        flush(live_all.at[: rows - 1], m_send)
        pl.when(distant)(lambda: flush(some.at[:2], l_send.at[0]))
        count_a = jnp.logical_and(nearby, jnp.logical_not(crosses[0]))
        count_b = jnp.logical_and(nearby, crosses[0])
        pl.when(count_a)(lambda: flush(u_ref.at[0, : 7 * lines // 2], l_send.at[0]))
        pl.when(count_b)(lambda: flush(some.at[: rows - 1, 0], l_send.at[0]))
        pl.when(count_b)(lambda: flush(some.at[0, 0], l_send.at[1]))
        single = jnp.logical_and(count_a, jnp.logical_not(opener))
        pl.when(single)(place(1, 0).wait_send)
        pl.when(late)(lambda: flush(some.at[:2], g_send))
        pl.when(helps[0])(lambda: flush(some.at[:2], c_send))
        only = jnp.logical_and(helps[1], jnp.logical_not(helps[0]))
        pl.when(only)(lambda: flush(some.at[0], c_send))

        @pl.when(gate)
        def _():
            flush(l_all, relay_send)

            @pl.when(jnp.logical_and(at_end, entry))
            def _():
                for h in range(2):
                    flush(some.at[:rows], post_send.at[h])

            @pl.when(jnp.logical_and(inner, entry))
            def _():
                flush(some.at[:3], post_send.at[0])
                flush(some.at[:2], post_send.at[1])

            @pl.when(jnp.logical_and(inner, second))
            def _():
                flush(some.at[0], post_send.at[0])
                flush(some.at[:2], post_send.at[1])

    def inner_step(k):
        if k == 3:
            ahead(0, across_mid, other)
            ahead(0, far_end, other)
        if k == 5:
            ahead(1, far_end, other)
            ahead(0, far_end, g)
            back(0, other)
        if k == 6:
            collect(0, other, inward)
            collect(0, other, outward)
            trade(0)
            ahead(1, far_end, g)
            back(1, other)
        if k == 7:
            ahead(1, across_mid, other)
            back(0, g)
            ahead(0, across_mid, g)
            back(1, g)
            collect(1, other, inward)
            collect(1, other, outward)
            trade(1)
            ahead(1, across_mid, g)
            settle()
            collect(0, g, outward)
            collect(0, g, inward)
            finish(0)
            collect(1, g, outward)
            collect(1, g, inward)

    def body(k, carry):
        for h in range(2):
            take(k, range(2 * h, 2 * h + 2))
            item(k, halves[h])
        for step in range(levels * rows):
            @pl.when(k == step)
            def _(step=step):
                pl.when(at_end)(lambda: edge_step(step))
                shared_step(step)
                pl.when(inner)(lambda: inner_step(step))

        return carry

    lax.fori_loop(0, levels * rows, body, 0)

    @pl.when(at_end)
    def _():
        collect(0, other, outward)
        trade(0)
        collect(1, other, outward)
        trade(1)
        collect(0, g, outward)
        settle()
        finish(0)
        collect(1, g, outward)

    finish(1)
    flush(p_in.at[:, : rows - 1], p_send)
    flush(y_out, y_send)


def stationary(rows, cols, layers, lpanel, upanel, rowmap, colmap, blockmask, front_blocks):
    levels, _, width, depth = lpanel.shape
    bf16 = jnp.bfloat16
    vmem = pl.BlockSpec(memory_space=pltpu.VMEM)
    hbm = pl.BlockSpec(memory_space=pl.ANY)
    dma = pltpu.SemaphoreType.DMA
    return pl.pallas_call(
        functools.partial(kernel, rows, cols, layers, levels, width),
        out_shape=pltpu.VMEM(front_blocks.shape, front_blocks.dtype),
        in_specs=[hbm] * 6,
        out_specs=vmem,
        scratch_shapes=[
            pltpu.VMEM(colmap.shape, jnp.int32),
            pltpu.VMEM((1, 1, levels), jnp.int32),
            pltpu.VMEM((levels, width, depth), bf16),
            pltpu.VMEM(upanel[:, 0].shape, bf16),
            pltpu.VMEM(front_blocks.shape, bf16),
            pltpu.VMEM((levels, width, depth), bf16),
            pltpu.VMEM((levels, width, depth), bf16),
            pltpu.VMEM((levels, rows, width, depth), bf16),
            pltpu.VMEM((rows,) + blockmask.shape[:1] + blockmask.shape[2:], jnp.int32),
            pltpu.VMEM((levels, rows, layers, width, width), jnp.float32),
            pltpu.VMEM((levels, rows, layers, width, width), bf16),
            pltpu.VMEM((levels, rows + 1, layers, width, width), bf16),
            pltpu.VMEM((levels, width, width), bf16),
            pltpu.VMEM((levels, width, width), bf16),
            pltpu.VMEM((1, 1, levels), jnp.int32),
            dma((6,)),
            dma,
            dma((levels, 2)),
            dma,
            dma((2,)),
            dma((levels, 4, rows)),
            dma((2,)),
            dma,
            dma,
            dma,
            dma,
            dma((levels, rows + 1, layers)),
            dma,
            dma((levels,)),
            dma,
            dma,
            pltpu.SemaphoreType.REGULAR,
            dma((levels,)),
            dma,
        ],
        compiler_params=pltpu.CompilerParams(collective_id=0, has_side_effects=True),
    )(
        lpanel[:, 0], upanel[:, 0], colmap, blockmask[:, 0], jnp.transpose(rowmap, (1, 2, 0)),
        front_blocks,
    )


def solution(mesh):
    rows, cols, layers = mesh.shape["row"], mesh.shape["col"], mesh.shape["gz"]
    body = general
    if rows == cols == 2 * layers and layers == 2:
        body = functools.partial(stationary, rows, cols, layers)
    return jax.shard_map(
        body,
        mesh=mesh,
        in_specs=(
            P(None, "gz", "row", "col"),
            P(None, "gz", "row", "col"),
            P(None, "gz", "row"),
            P(None, "gz", "col"),
            P(None, "gz", "row", "col"),
            P(None, "row", ("gz", "col")),
        ),
        out_specs=P(None, "row", ("gz", "col")),
        check_vma=False,
    )
```

```python
import functools

import jax
import jax.numpy as jnp
from jax import lax
from jax.experimental import pallas as pl
from jax.experimental.pallas import tpu as pltpu
from jax.sharding import PartitionSpec as P

CB = 4
FRB = 2
MESH = pl.DeviceIdType.MESH


def column_sums(schur, cols_of, live, layers):
    width = schur.shape[0]
    blocks = schur.reshape(width, CB, width)
    targets = cols_of[:, None] == jnp.arange(layers, dtype=jnp.int32)[None, :]
    col_select = targets.astype(jnp.float32) * live.astype(jnp.float32)[:, None]
    return jnp.einsum("bjk,jl->lbk", blocks, col_select, precision=lax.Precision.HIGHEST)


def general(lpanel, upanel, rowmap, colmap, blockmask, front_blocks):
    layers = lax.axis_size("gz")
    width = lpanel.shape[2]
    levels = lpanel.shape[0]
    tiles = []
    for depth in range(levels):
        left_rows = lax.all_gather(lpanel[depth, 0], "col", axis=1, tiled=True)
        tiles.append(
            jnp.dot(
                left_rows,
                lax.all_gather(upanel[depth, 0], "row", axis=0, tiled=True),
                preferred_element_type=jnp.float32,
            )
        )
    results = []
    every_row = lax.all_gather(rowmap[:, :, 0], "gz", axis=1, tiled=True)
    for depth in range(levels):
        sums = column_sums(tiles[depth], colmap[depth, 0], blockmask[depth, 0, 0], layers).astype(
            jnp.bfloat16
        )
        arrived = lax.all_to_all(sums, "gz", split_axis=0, concat_axis=0, tiled=True)
        row_select = (
            every_row[depth][:, None] == jnp.arange(FRB, dtype=jnp.int32)[None, :]
        ).astype(jnp.float32)
        placed = jnp.einsum(
            "sf,sbk->fbk", row_select, arrived.astype(jnp.float32), precision=lax.Precision.HIGHEST
        )
        placed = placed.reshape(FRB * width, width)
        results.append((front_blocks[depth].astype(jnp.float32) - placed).astype(jnp.bfloat16))
    return jnp.stack(results)


def kernel(
    rows, cols, layers, levels, width,
    l_hbm, u_hbm, cm_hbm, live_hbm, rm_hbm, front_hbm, out_ref,
    cm_ref, rm_ref,
    l_ref, u_ref, front_ref, crossed, stash, l_all, live_all, own, part, p_in, y_out, y_in, rm_in,
    in_sem, own_sem, x_recv, c_send, l_send, l_recv, post_send, relay_send,
    m_send, m_recv, p_send, p_recv, y_send, y_recv, rm_send, rm_recv, turn, f_recv, g_send,
):
    z = lax.axis_index("row")
    c = lax.axis_index("col")
    g = lax.axis_index("gz")
    far = lax.rem(c + cols // 2, cols)
    mate = c + 1 - 2 * lax.rem(c, 2)
    other = 1 - g
    last = rows - 1
    entry, second = c == z, far == z
    gate = jnp.logical_or(entry, second)
    low = 1 - z // (rows // 2)
    depth = low * z + (1 - low) * (last - z)
    at_end = depth == 0
    inner = jnp.logical_not(at_end)

    def remote(src, dst, send, recv, where):
        return pltpu.make_async_remote_copy(
            src_ref=src, dst_ref=dst, send_sem=send, recv_sem=recv,
            device_id=where, device_id_type=MESH,
        )

    barrier = pltpu.get_barrier_semaphore()
    for step in range(1, rows):
        pl.semaphore_signal(
            barrier, inc=1, device_id={"row": lax.rem(z + step, rows)}, device_id_type=MESH
        )
    pl.semaphore_signal(barrier, inc=1, device_id={"col": far}, device_id_type=MESH)
    pl.semaphore_signal(barrier, inc=1, device_id={"col": mate}, device_id_type=MESH)
    pl.semaphore_signal(barrier, inc=1, device_id={"gz": other}, device_id_type=MESH)

    first = pltpu.make_async_copy(l_hbm, l_ref, in_sem.at[0])
    first.start()
    small = [
        pltpu.make_async_copy(src, dst, in_sem.at[3 + i])
        for i, (src, dst) in enumerate(
            ((live_hbm, live_all.at[z]), (rm_hbm, rm_ref), (cm_hbm, cm_ref))
        )
    ]
    for copy in small:
        copy.start()
    whole_u = pltpu.make_async_copy(u_hbm, u_ref, in_sem.at[1])
    whole_u.start()
    fronts = pltpu.make_async_copy(front_hbm, front_ref, in_sem.at[2])
    fronts.start()

    own_load = pltpu.make_async_copy(l_hbm, l_all.at[:, z], own_sem)
    pl.when(entry)(own_load.start)

    for copy in small:
        copy.wait()
    first.wait()
    pl.semaphore_wait(barrier, rows + 2)

    parts = 4
    lines = width // parts
    pieces = [slice(h * lines, (h + 1) * lines) for h in range(parts)]
    halves = [slice(h * 2 * lines, (h + 1) * 2 * lines) for h in range(2)]

    def place(v, h):
        return remote(
            l_ref.at[v, pieces[h]], l_all.at[v, z, pieces[h]],
            l_send.at[int(v == 1 and h == 0)], l_recv.at[v, h, z], {"row": c},
        )

    def cross(v, h):
        return remote(
            l_ref.at[v, halves[h]], crossed.at[v, halves[h]],
            l_send.at[v * (1 - h)], x_recv.at[v, h], {"col": far},
        )

    def onward(v, h):
        return remote(
            crossed.at[v, pieces[h]], l_all.at[v, z, pieces[h]],
            c_send, l_recv.at[v, h, z], {"row": far},
        )

    def routes(q):
        central = q * (last - q) > 0
        both = jnp.logical_and(jnp.logical_and(inner, central), q != z)
        one = jnp.logical_and(jnp.logical_and(at_end, central), (q - z) * (q - z) == 4)
        return both, jnp.logical_or(both, one)

    away = jnp.logical_not(entry)
    crosses, helps = routes(c), routes(far)
    places = [jnp.logical_and(away, jnp.logical_not(flag)) for flag in crosses]

    def launch(v):
        for h in range(2):
            pl.when(crosses[h])(lambda h=h: cross(v, h).start())
        for h in range(parts):
            pl.when(places[h // 2])(lambda h=h: place(v, h).start())

    def carry_on(v):
        for h in range(2):
            @pl.when(helps[h])
            def _(h=h):
                cross(v, h).wait_recv()
                for n in range(2):
                    onward(v, 2 * h + n).start()

    live_out = []
    for step in range(1, rows):
        to = lax.rem(z + step, rows)
        live_out.append(remote(live_all.at[z], live_all.at[z], m_send, m_recv, {"row": to}))
        live_out[-1].start()
    rm_copy = remote(rm_ref, rm_in, rm_send, rm_recv, {"gz": other})
    rm_copy.start()
    gap = (z - c) * (z - c)
    to_end = c * (last - c) == 0
    distant = gap == 9
    late = jnp.logical_and(inner, jnp.logical_and(gap == 4, to_end))
    opener = jnp.logical_and(inner, jnp.logical_and(gap == 1, to_end))
    nearby = jnp.logical_and(away, jnp.logical_not(distant))
    lead = jnp.logical_and(nearby, jnp.logical_not(late))
    near_end, far_end = last * (1 - low), last * low
    next_in = low + (1 - low) * (last - 1)

    def deposit(v):
        return remote(l_ref.at[v], stash.at[v], l_send.at[0], f_recv.at[v], {"row": next_in})

    def pick_up(v, h):
        return remote(
            stash.at[v, pieces[h]], l_all.at[v, near_end, pieces[h]],
            g_send, l_recv.at[v, h, near_end], {"row": c},
        )

    @pl.when(distant)
    def _():
        for v in range(levels):
            deposit(v).start()

    @pl.when(lead)
    def _():
        for v in range(levels):
            launch(v)

    @pl.when(opener)
    def _():
        place(1, 0).wait_send()
        pl.semaphore_signal(turn, inc=1, device_id={"row": last - z}, device_id_type=MESH)

    @pl.when(late)
    def _():
        pl.semaphore_wait(turn, 1)
        launch(0)
        for v in range(levels):
            deposit(v).wait_recv()
            for h in range(parts):
                pick_up(v, h).start()
        launch(1)

    def passes(v, a, h):
        spot = l_all.at[v, a, pieces[h]]
        post = remote(spot, spot, post_send.at[h // 2], l_recv.at[v, h, a], {"col": far})
        relay = remote(spot, spot, relay_send, l_recv.at[v, h, a], {"col": mate})
        return post, relay

    count = rows - 1

    def place_of(k):
        mine = k // (levels * count)
        first = 1 - (k + levels) // (2 * levels)
        rest = k - levels
        v = first * k + (1 - first) * (rest // levels)
        step = lax.rem(rest + 2 * levels, levels)
        i = (1 - first) * (1 + step + v * (1 - 2 * step))
        near = (1 - depth) * (i + 1) + depth * (i + (i + 1) // 2)
        near = low * near + (1 - low) * (last - near)
        v = mine * (k - levels * count) + (1 - mine) * v
        return v, mine * z + (1 - mine) * near

    def turned(v, a, h):
        both = a == last - z
        return jnp.logical_and(inner, both if h < 2 else jnp.logical_or(both, (a - z) * (a - z) == 4))

    def spread(v, a, h):
        post, relay = passes(v, a, h)
        post.start()
        relay.start()

    def gather_entry(k):
        v, a = place_of(k)

        @pl.when(entry)
        def _():
            if k == levels * count:
                own_load.wait()
            for h in range(parts):
                @pl.when(jnp.logical_not(turned(v, a, h)))
                def _(h=h):
                    pl.when(a != z)(lambda: passes(v, a, h)[1].wait_recv())
                    spread(v, a, h)

    def gather_second(k):
        v, a = place_of(k)
        for h in range(parts):
            @pl.when(jnp.logical_and(second, turned(v, a, h)))
            def _(h=h):
                passes(v, a, h)[1].wait_recv()
                spread(v, a, h)

    def gather(k):
        gather_entry(k)
        gather_second(k)

    def take(k, part_of):
        v, a = place_of(k)

        def hand(h):
            relay = passes(v, a, h)[1]
            relay.wait_recv()
            relay.start()

        for h in part_of:
            there = turned(v, a, h)
            taken = jnp.logical_or(
                jnp.logical_and(second, jnp.logical_not(there)), jnp.logical_and(entry, there)
            )
            pl.when(taken)(lambda h=h: hand(h))

        @pl.when(jnp.logical_not(gate))
        def _():
            for h in part_of:
                passes(v, a, h)[1].wait_recv()

    def hop(v, a, l, side, row, to):
        slot = a + (rows - a) * side * (a == row).astype(jnp.int32)
        return remote(
            part.at[v, a, l], p_in.at[v, slot, l], p_send, p_recv.at[v, slot, l], {"row": to}
        )

    inward, outward = 1 - low, low
    across_mid = last - z

    def send(v, a, l):
        part[v, a, l] = own[v, a, l].astype(jnp.bfloat16)
        hop(v, a, l, inward, next_in, next_in).start()

    def item(k, lane):
        v, a = place_of(k)
        block = l_all[v, a, lane, :]
        to_layer = cm_ref[v]
        live = live_all[a, v]
        for j in range(CB):
            t = jnp.dot(
                block, u_ref[v, :, j * width : (j + 1) * width], preferred_element_type=jnp.float32
            )
            for l in range(layers):
                m = jnp.where(to_layer[:, j : j + 1] == l, live[:, j : j + 1], 0).astype(jnp.float32)
                if j == 0:
                    own[v, a, l, lane, :] = t * m
                else:
                    own[v, a, l, lane, :] += t * m

    gather_entry(0)
    carry_on(0)

    @pl.when(inner)
    def _():
        gather_entry(1)
        carry_on(1)
        gather(2)

    def flush(ref, sem):
        pltpu.make_async_copy(ref, ref, sem).wait()

    flush(live_all.at[: rows - 1], m_recv)
    whole_u.wait()
    rm_copy.wait()
    fronts.wait()

    def taken_in(v, a, l, side):
        slot = a + (rows - a) * side * (a == z).astype(jnp.int32)
        hop(v, a, l, side, z, z).wait_recv()
        return p_in[v, slot, l].astype(jnp.float32)

    def collect(v, l, side):
        own[v, z, l] += taken_in(v, z, l, side)

    def forward(v, a, l, side, to):
        part[v, a, l] = (own[v, a, l] + taken_in(v, a, l, side)).astype(jnp.bfloat16)
        hop(v, a, l, side, to, to).start()

    def way(v):
        return remote(y_out.at[v], y_in.at[v], y_send, y_recv.at[v], {"gz": other})

    def trade(v):
        y_out[v] = own[v, z, other].astype(jnp.bfloat16)
        way(v).start()

    def finish(v):
        mine = own[v, z, g].astype(jnp.bfloat16).astype(jnp.float32)
        way(v).wait_recv()
        theirs = y_in[v].astype(jnp.float32)
        for f in range(FRB):
            lines = slice(f * width, (f + 1) * width)
            here = (rm_ref[0, :, v : v + 1] == f).astype(jnp.float32)
            there = (rm_in[0, :, v : v + 1] == f).astype(jnp.float32)
            total = here * mine + there * theirs
            out_ref[v, lines, :] = (front_ref[v, lines, :].astype(jnp.float32) - total).astype(
                out_ref.dtype
            )


    def ahead(v, a, l):
        forward(v, a, l, inward, across_mid)

    def back(v, l):
        forward(v, near_end, l, outward, near_end)

    near, mid, end = next_in, last - next_in, last - z
    early = {
        0: ((0, near, other),),
        1: ((1, near, other),),
        2: ((0, mid, other),),
        3: ((0, end, other),),
        4: ((1, end, other), (0, end, g), (1, end, g)),
        5: ((1, mid, other), (0, mid, g), (1, mid, g), (0, near, g), (1, near, g)),
    }

    def edge_step(k):
        for v, a, l in early.get(k, ()):
            send(v, a, l)

    def edge_gather(k):
        if k < 5:
            gather_entry(k + 1)
        if k == 0:
            carry_on(1)
        if k == 5:
            gather_entry(6)
            gather_entry(7)

    def inner_gather(k):
        if k < 3:
            gather(k + 3)
        if k == 3:
            gather_entry(6)
            gather_entry(7)

    def shared_step(k):
        pl.when(at_end)(lambda: edge_gather(k))
        pl.when(inner)(lambda: inner_gather(k))

    def settle():
        some = p_in.at[0]
        flush(live_all.at[: rows - 1], m_send)
        pl.when(distant)(lambda: flush(some.at[:2], l_send.at[0]))
        count_a = jnp.logical_and(nearby, jnp.logical_not(crosses[0]))
        count_b = jnp.logical_and(nearby, crosses[0])
        pl.when(count_a)(lambda: flush(u_ref.at[0, : 7 * lines // 2], l_send.at[0]))
        pl.when(count_b)(lambda: flush(some.at[: rows - 1, 0], l_send.at[0]))
        pl.when(count_b)(lambda: flush(some.at[0, 0], l_send.at[1]))
        single = jnp.logical_and(count_a, jnp.logical_not(opener))
        pl.when(single)(place(1, 0).wait_send)
        pl.when(late)(lambda: flush(some.at[:2], g_send))
        pl.when(helps[0])(lambda: flush(some.at[:2], c_send))
        only = jnp.logical_and(helps[1], jnp.logical_not(helps[0]))
        pl.when(only)(lambda: flush(some.at[0], c_send))

        @pl.when(gate)
        def _():
            flush(l_all, relay_send)

            @pl.when(jnp.logical_and(at_end, entry))
            def _():
                for h in range(2):
                    flush(some.at[:rows], post_send.at[h])

            @pl.when(jnp.logical_and(inner, entry))
            def _():
                flush(some.at[:3], post_send.at[0])
                flush(some.at[:2], post_send.at[1])

            @pl.when(jnp.logical_and(inner, second))
            def _():
                flush(some.at[0], post_send.at[0])
                flush(some.at[:2], post_send.at[1])

    def inner_step(k):
        if k == 3:
            ahead(0, across_mid, other)
            ahead(0, far_end, other)
        if k == 5:
            ahead(1, far_end, other)
            ahead(0, far_end, g)
            back(0, other)
        if k == 6:
            collect(0, other, inward)
            collect(0, other, outward)
            trade(0)
            ahead(1, far_end, g)
            back(1, other)
        if k == 7:
            ahead(1, across_mid, other)
            back(0, g)
            ahead(0, across_mid, g)
            back(1, g)
            collect(1, other, inward)
            collect(1, other, outward)
            trade(1)
            ahead(1, across_mid, g)
            settle()
            collect(0, g, outward)
            collect(0, g, inward)
            finish(0)
            collect(1, g, outward)
            collect(1, g, inward)

    def body(k, carry):
        take(k, range(2))
        item(k, halves[0])
        for h in range(2, parts):
            take(k, range(h, h + 1))
            item(k, pieces[h])
        for step in range(levels * rows):
            @pl.when(k == step)
            def _(step=step):
                pl.when(at_end)(lambda: edge_step(step))
                shared_step(step)
                pl.when(inner)(lambda: inner_step(step))

        return carry

    lax.fori_loop(0, levels * rows, body, 0)

    @pl.when(at_end)
    def _():
        collect(0, other, outward)
        trade(0)
        collect(1, other, outward)
        trade(1)
        collect(0, g, outward)
        settle()
        finish(0)
        collect(1, g, outward)

    finish(1)
    flush(p_in.at[:, : rows - 1], p_send)
    flush(y_out, y_send)


def stationary(rows, cols, layers, lpanel, upanel, rowmap, colmap, blockmask, front_blocks):
    levels, _, width, depth = lpanel.shape
    bf16 = jnp.bfloat16
    vmem = pl.BlockSpec(memory_space=pltpu.VMEM)
    hbm = pl.BlockSpec(memory_space=pl.ANY)
    dma = pltpu.SemaphoreType.DMA
    return pl.pallas_call(
        functools.partial(kernel, rows, cols, layers, levels, width),
        out_shape=pltpu.VMEM(front_blocks.shape, front_blocks.dtype),
        in_specs=[hbm] * 6,
        out_specs=vmem,
        scratch_shapes=[
            pltpu.VMEM(colmap.shape, jnp.int32),
            pltpu.VMEM((1, 1, levels), jnp.int32),
            pltpu.VMEM((levels, width, depth), bf16),
            pltpu.VMEM(upanel[:, 0].shape, bf16),
            pltpu.VMEM(front_blocks.shape, bf16),
            pltpu.VMEM((levels, width, depth), bf16),
            pltpu.VMEM((levels, width, depth), bf16),
            pltpu.VMEM((levels, rows, width, depth), bf16),
            pltpu.VMEM((rows,) + blockmask.shape[:1] + blockmask.shape[2:], jnp.int32),
            pltpu.VMEM((levels, rows, layers, width, width), jnp.float32),
            pltpu.VMEM((levels, rows, layers, width, width), bf16),
            pltpu.VMEM((levels, rows + 1, layers, width, width), bf16),
            pltpu.VMEM((levels, width, width), bf16),
            pltpu.VMEM((levels, width, width), bf16),
            pltpu.VMEM((1, 1, levels), jnp.int32),
            dma((6,)),
            dma,
            dma((levels, 2)),
            dma,
            dma((2,)),
            dma((levels, 4, rows)),
            dma((2,)),
            dma,
            dma,
            dma,
            dma,
            dma((levels, rows + 1, layers)),
            dma,
            dma((levels,)),
            dma,
            dma,
            pltpu.SemaphoreType.REGULAR,
            dma((levels,)),
            dma,
        ],
        compiler_params=pltpu.CompilerParams(collective_id=0, has_side_effects=True),
    )(
        lpanel[:, 0], upanel[:, 0], colmap, blockmask[:, 0], jnp.transpose(rowmap, (1, 2, 0)),
        front_blocks,
    )


def solution(mesh):
    rows, cols, layers = mesh.shape["row"], mesh.shape["col"], mesh.shape["gz"]
    body = general
    if rows == cols == 2 * layers and layers == 2:
        body = functools.partial(stationary, rows, cols, layers)
    return jax.shard_map(
        body,
        mesh=mesh,
        in_specs=(
            P(None, "gz", "row", "col"),
            P(None, "gz", "row", "col"),
            P(None, "gz", "row"),
            P(None, "gz", "col"),
            P(None, "gz", "row", "col"),
            P(None, "row", ("gz", "col")),
        ),
        out_specs=P(None, "row", ("gz", "col")),
        check_vma=False,
    )
```
